32 devices in a mesh: frame: 4 (over x, core), fsdp: 4 (over z), head: 2 (over y).
Axes of the slice: x: 2, y: 2, z: 4, core: 2. Of those that a mesh axis runs over, the one named last changes fastest.
Arguments:
- queries: bfloat16 [1024, 10240], P('frame', ('fsdp', 'head')), may hold values from -6 to 6
- noisy_keys: bfloat16 [1024, 10240], P('frame', ('fsdp', 'head')), may hold values from -6 to 6
- noisy_values: bfloat16 [1024, 10240], P('frame', ('fsdp', 'head')), may hold values from -6 to 6
- clean_keys: bfloat16 [1024, 10240], P('frame', ('fsdp', 'head')), may hold values from -10 to 10
- clean_values: bfloat16 [1024, 10240], P('frame', ('fsdp', 'head')), may hold values from -6 to 6
- gain_query: float32 [5120], replicated, may hold values from 0.5 to 2
- gain_key: float32 [5120], replicated, may hold values from 0.5 to 2
- out_grad: bfloat16 [1024, 10240], P('frame', ('fsdp', 'head')), may hold values from -6 to 6
Outputs:
- attended: bfloat16 [1024, 10240], P('frame', ('fsdp', 'head'))
- grad_queries: bfloat16 [1024, 10240], P('frame', ('fsdp', 'head'))
- grad_keys: bfloat16 [1024, 10240], P('frame', ('fsdp', 'head'))
- grad_values: bfloat16 [1024, 10240], P('frame', ('fsdp', 'head'))
- grad_gain_query: float32 [5120], replicated
- grad_gain_key: float32 [5120], replicated
The draws below stay inside these ranges and needn't reach their ends.
All inputs are finite; a program needn't handle non-finite values.
Results may differ from the reference program's by a relative error of at most 0.012.
Values may be sent and summed in bfloat16 or wider, within the bound.
A program may use at most 64 MiB of HBM per device.

```python
import math
import jax
import jax.numpy as jnp
from jax import lax

D = 5120
HEADS = 40
DH = 128
FRAME_TOK = 256
FRAMES = 4
SEQ = 1024
VIDEOS = 2


def half_scales(key, salt):
    lowest = math.log(0.2)
    drawn = jax.random.uniform(jax.random.fold_in(key, salt), (SEQ, VIDEOS, 2), jnp.float32, lowest, 0.0)
    scales = jnp.exp(drawn)
    columns = jnp.arange(VIDEOS * D)
    video_of = columns % (VIDEOS * D // 2) // (D // 2)
    half_of = columns // (VIDEOS * D // 2)
    return scales[:, video_of, half_of]


def draw_queries(key, part):
    base = jnp.clip(jax.random.normal(jax.random.fold_in(key, 11), (SEQ, VIDEOS * D), jnp.float32), -6.0, 6.0)
    base = base * half_scales(key, 4411)
    return base.astype(jnp.bfloat16)


def draw_noisy_keys(key, part):
    base = jnp.clip(jax.random.normal(jax.random.fold_in(key, 13), (SEQ, VIDEOS * D), jnp.float32), -6.0, 6.0)
    base = base * half_scales(key, 4413)
    return base.astype(jnp.bfloat16)


def draw_clean_keys(key, part):
    base = jnp.clip(jax.random.normal(jax.random.fold_in(key, 12), (SEQ, VIDEOS * D), jnp.float32), -6.0, 6.0)
    return base.astype(jnp.bfloat16)


def block_levels(key, extent, shards, smallest, top_value):
    level = 1.0
    for dim, shards_of in shards:
        draws = jax.random.uniform(jax.random.fold_in(jax.random.fold_in(key, 6), dim), (shards_of,), jnp.float32, smallest / len(shards), top_value / len(shards))
        level = level * jnp.repeat(jnp.exp(draws), extent[dim] // shards_of).reshape((-1,) + (1,) * (len(extent) - 1 - dim))
    return level


def normal_values(rng, extent, width, bound, pieces=(), kind=jnp.bfloat16):
    level = block_levels(rng, extent, pieces, -0.22, 0.18) if pieces else 1.0
    values = jax.random.normal(rng, extent, jnp.float32) * width * level
    return jnp.minimum(jnp.maximum(values, -bound), bound).astype(kind)


def setup_inputs(seed: int = 0) -> dict:
    keys = jax.random.split(jax.random.key(seed), 9)
    queries = draw_queries(jax.random.fold_in(keys[8], 71), 0)
    noisy_keys = draw_noisy_keys(jax.random.fold_in(keys[8], 71), 0)
    noisy_values = normal_values(keys[2], (SEQ, VIDEOS * D), 1.0, 6.0, ((0, 4), (1, 8)))
    clean_keys = draw_clean_keys(jax.random.fold_in(keys[8], 71), 0)
    clean_values = normal_values(keys[4], (SEQ, VIDEOS * D), 1.0, 6.0, ((0, 4), (1, 8)))
    gain_query = jnp.clip(jnp.exp(jax.random.uniform(keys[5], (D,), jnp.float32, math.log(0.5), math.log(2.0))), 0.5, 2.0)
    gain_key = jnp.clip(jnp.exp(jax.random.uniform(keys[6], (D,), jnp.float32, math.log(0.5), math.log(2.0))), 0.5, 2.0)
    out_grad = normal_values(keys[7], (SEQ, VIDEOS * D), 1.0, 6.0, ((0, 4), (1, 8)))
    return {"queries": queries, "noisy_keys": noisy_keys, "noisy_values": noisy_values, "clean_keys": clean_keys, "clean_values": clean_values, "gain_query": gain_query, "gain_key": gain_key, "out_grad": out_grad}


EPSILON = 1e-06

def rounded(values_in):
    return lax.optimization_barrier(values_in.astype(jnp.bfloat16)).astype(jnp.float32)

def normalize(raw, gain):
    full = raw.astype(jnp.float32)
    rate = lax.rsqrt(lax.optimization_barrier(jnp.mean(full * full, axis=1)) + EPSILON)
    return (full, rate, (full * rate[:, None] * gain).astype(jnp.bfloat16))

def norm_grad(full, rate, gain, grad_normed):
    flat = grad_normed * gain
    inner = lax.optimization_barrier(jnp.sum(full * flat, axis=1))
    grad_raw = rate[:, None] * flat - full * (rate * rate * rate * inner / D)[:, None]
    grad_gain = lax.optimization_barrier(jnp.sum(grad_normed * full * rate[:, None], axis=0))
    return (grad_raw.astype(jnp.bfloat16), grad_gain)

def by_video(array):
    split = array.reshape(SEQ, 2, VIDEOS, D // 2)
    return jnp.transpose(split, (2, 0, 1, 3)).reshape(VIDEOS, SEQ, D)

def by_column(array):
    split = array.reshape(VIDEOS, SEQ, 2, D // 2)
    return jnp.transpose(split, (1, 2, 0, 3)).reshape(SEQ, VIDEOS * D)

def reference(queries, noisy_keys, noisy_values, clean_keys, clean_values, gain_query, gain_key, out_grad):
    scaling = 1.0 / math.sqrt(DH)
    highest = lax.Precision.HIGHEST

    def one_video(inputs):
        video_q, video_k, video_v, video_ck, video_cv, video_g = inputs
        q_full, rate_q, normed_q = normalize(video_q, gain_query)
        k_full, rate_k, normed_k = normalize(video_k, gain_key)
        outputs, grads_q, grads_k, grads_v = ([], [], [], [])
        for frame_index in range(FRAMES):
            first_row = frame_index * FRAME_TOK
            last_row = first_row + FRAME_TOK
            query_f = normed_q[first_row:last_row].astype(jnp.float32).reshape(FRAME_TOK, HEADS, DH)
            key_all = jnp.concatenate([normed_k[first_row:last_row], video_ck[:first_row]], axis=0)
            key_all = key_all.astype(jnp.float32).reshape(-1, HEADS, DH)
            value_all = jnp.concatenate([video_v[first_row:last_row], video_cv[:first_row]], axis=0)
            value_all = value_all.astype(jnp.float32).reshape(-1, HEADS, DH)
            grad_out = video_g[first_row:last_row].astype(jnp.float32).reshape(FRAME_TOK, HEADS, DH)
            scores = jnp.einsum('qhd,khd->hqk', query_f, key_all, precision=highest) * scaling
            row_max = lax.optimization_barrier(jnp.max(scores, axis=2))
            expo = jnp.exp(scores - row_max[:, :, None])
            total = lax.optimization_barrier(jnp.sum(expo, axis=2))
            summed = jnp.einsum('hqk,khd->qhd', rounded(expo), value_all, precision=highest)
            attention_f32 = summed / jnp.transpose(total)[:, :, None]
            log_total = row_max + jnp.log(total)
            soft_probs = jnp.exp(scores - log_total[:, :, None])
            delta = jnp.transpose(lax.optimization_barrier(jnp.sum(grad_out * attention_f32, axis=2)))
            grad_probs = jnp.einsum('qhd,khd->hqk', grad_out, value_all, precision=highest)
            grad_scores = rounded(soft_probs * (grad_probs - delta[:, :, None]))
            grad_qn = jnp.einsum('hqk,khd->qhd', grad_scores, key_all, precision=highest) * scaling
            grad_kn = jnp.einsum('hqk,qhd->khd', grad_scores[:, :, :FRAME_TOK], query_f, precision=highest) * scaling
            grad_vv = jnp.einsum('hqk,qhd->khd', rounded(soft_probs[:, :, :FRAME_TOK]), grad_out, precision=highest)
            outputs.append(attention_f32.reshape(FRAME_TOK, D).astype(jnp.bfloat16))
            grads_q.append(grad_qn.reshape(FRAME_TOK, D))
            grads_k.append(grad_kn.reshape(FRAME_TOK, D))
            grads_v.append(grad_vv.reshape(FRAME_TOK, D).astype(jnp.bfloat16))
        grad_q_raw, gain_q_part = norm_grad(q_full, rate_q, gain_query, jnp.concatenate(grads_q, axis=0))
        grad_k_raw, gain_k_part = norm_grad(k_full, rate_k, gain_key, jnp.concatenate(grads_k, axis=0))
        return (jnp.concatenate(outputs, axis=0), grad_q_raw, grad_k_raw, jnp.concatenate(grads_v, axis=0), gain_q_part, gain_k_part)
    stacked = tuple((by_video(member) for member in (queries, noisy_keys, noisy_values, clean_keys, clean_values, out_grad)))
    results = lax.map(one_video, stacked)
    attended, grad_queries, grad_keys, grad_values, gain_q_parts, gain_k_parts = results
    return (by_column(attended), by_column(grad_queries), by_column(grad_keys), by_column(grad_values), lax.optimization_barrier(jnp.sum(gain_q_parts, axis=0)), lax.optimization_barrier(jnp.sum(gain_k_parts, axis=0)))
```

```python
import functools
import math

import jax
import jax.numpy as jnp
from jax import lax
from jax.experimental import pallas as pl
from jax.experimental.pallas import tpu as pltpu
from jax.sharding import PartitionSpec as P

DH = 128
EPSILON = 1e-06
MESH = pl.DeviceIdType.MESH
VMEM_BYTES = 67043328
F32 = jnp.float32
BF16 = jnp.bfloat16


def dot_nt(a, b):
    return lax.dot_general(a, b, (((1,), (1,)), ((), ())), preferred_element_type=F32)


def dot_nn(a, b):
    return lax.dot_general(a, b, (((1,), (0,)), ((), ())), preferred_element_type=F32)


def dot_tn(a, b):
    return lax.dot_general(a, b, (((0,), (0,)), ((), ())), preferred_element_type=F32)


def kernel(
    frames, fsdp, heads_axis, width, features, lent,
    q_hbm, k_hbm, v_hbm, ck_hbm, cv_hbm, gq_hbm, gk_hbm, g_hbm,
    att_out, dq_out, dk_out, dv_out, gain_q_out, gain_k_out,
    q, k, v, g, gq, gk, cks, cvs, flat_q, flat_k, inner_q, inner_k, rates,
    stats, sums1, sums2, far_q, far_g, far_rates, far_inner, part, back_out, back_in,
    near_trip, far_trip, trip_out, trip_in, row_out, row_in,
    load_sem, own_send, relay_send, clean_recv, stats_send, stats_recv, s1_send, s1_recv, s2_send, s2_recv,
    stage_sem, far_send, far_recv, back_send, back_recv, trip_send, trip_recv, row_send, row_recv,
):
    length = q.shape[0]
    head_count = width // DH
    kept = head_count - lent
    videos = fsdp // 2
    scaling = 1.0 / math.sqrt(DH)
    power = scaling * math.log2(math.e)
    frame = lax.axis_index("frame")
    fs = lax.axis_index("fsdp")
    half = fs // videos
    video = lax.rem(fs, videos)
    me1 = frame * videos + video
    n1 = frames * videos
    me2 = half * heads_axis + lax.axis_index("head")
    n2 = 2 * heads_axis

    def peer1(distance):
        p = lax.rem(me1 + distance, n1)
        return {"frame": p // videos, "fsdp": half * videos + lax.rem(p, videos)}

    def peer2(distance):
        p = lax.rem(me2 + distance, n2)
        return {"fsdp": (p // heads_axis) * videos + video, "head": lax.rem(p, heads_axis)}

    def columns(h):
        return pl.ds(pl.multiple_of(h * DH, DH), DH)

    def repeat(first, last, step):
        def body(i, _):
            step(i)
            return 0

        lax.fori_loop(first, last, body, 0)

    def stage_copy(nb, h, kv):
        cols = columns(h)
        return pltpu.make_async_copy(
            (ck_hbm, cv_hbm)[kv].at[:, cols], (cks, cvs)[kv].at[nb, :, cols], stage_sem.at[h, kv]
        )

    for nb in range(frames - 1):

        @pl.when(frame == nb)
        def _():
            def stage(h):
                for kv in range(2):
                    stage_copy(nb, h, kv).start()

            repeat(0, head_count, stage)

    barrier = pltpu.get_barrier_semaphore()

    def greet(d, _):
        pl.semaphore_signal(barrier, inc=1, device_id=peer1(d), device_id_type=MESH)
        return 0

    lax.fori_loop(1, n1, greet, 0)
    for d in range(1, n2):
        pl.semaphore_signal(barrier, inc=1, device_id=peer2(d), device_id_type=MESH)
    start = pl.multiple_of(me2 * width, DH)
    loads = []
    for i, (src, dst) in enumerate(
        (
            (q_hbm, q),
            (k_hbm, k),
            (gq_hbm.at[:, pl.ds(start, width)], gq),
            (gk_hbm.at[:, pl.ds(start, width)], gk),
            (v_hbm, v),
            (g_hbm, g),
        )
    ):
        copy = pltpu.make_async_copy(src, dst, load_sem.at[i])
        copy.start()
        loads.append(copy)
    pl.semaphore_wait(barrier, n1 - 1 + n2 - 1)

    def frame_copy(src, dst, send, recv, target):
        return pltpu.make_async_remote_copy(
            src_ref=src,
            dst_ref=dst,
            send_sem=send,
            recv_sem=recv,
            device_id={"frame": jnp.int32(target)},
            device_id_type=MESH,
        )

    def clean_copy(j, h, kv, target, sends):
        land = (cks, cvs)[kv].at[j, :, columns(h)]
        return frame_copy(land, land, sends.at[h, kv], clean_recv.at[j, h, kv], target)

    def plan(nb):
        pair, side = nb // 2, nb % 2
        partner, further = 2 * pair + 1 - side, nb + 2
        direct = [2 * c + side for c in range(pair)]
        relayed = [2 * c + 1 - side for c in range(pair)] + ([nb - 1] if side else [])
        own = ([(0, further)] if further < frames else []) + ([(1, partner)] if side == 0 else [])
        passes = [partner] + ([further] if further < frames else [])
        return direct, relayed, own, passes

    def helps(nb):
        return lent > 0 and nb < 2

    def helped(nb):
        return lent > 0 and nb >= 2

    def own_lists(nb):
        own = plan(nb)[2]
        if not helps(nb):
            return own, own, own
        return own, [o for o in own if o[0] == 1], [(1, 1 - nb)]

    def send_own(nb, h, targets):
        for kv in range(2):
            for t, target in targets:
                clean_copy(nb, h, kv, target, own_send.at[t]).start()

    def far_copy(kind, r, target):
        if kind == 0:
            src, land = q_hbm, far_q
        else:
            src, land = g_hbm, far_g
        return frame_copy(
            src.at[:, columns(kept + r)], land.at[r], far_send.at[kind, r], far_recv.at[kind, r], target
        )

    def back_copy(kind, r, target):
        return frame_copy(
            back_out.at[kind, r], back_in.at[kind, r], back_send.at[kind, r], back_recv.at[kind, r], target
        )

    def trip_copy(target):
        return frame_copy(trip_out, trip_in, trip_send.at[0], trip_recv.at[0], target)

    def row_copy(target):
        return frame_copy(row_out, row_in, row_send.at[0], row_recv.at[0], target)

    def lend(nb, first, last):
        def go(r):
            for kind in range(2):
                far_copy(kind, r, nb - 2).start()

        repeat(first, last, go)

    for nb in range(frames):
        full, late, lends = own_lists(nb)

        @pl.when(frame == nb)
        def _():
            if helped(nb):
                lend(nb, 0, lent // 2)
            if nb < frames - 1:

                def go(targets):
                    def step(h):
                        for kv in range(2):
                            stage_copy(nb, h, kv).wait()
                        send_own(nb, h, targets)

                    return step

                repeat(0, kept - 1, go(full))
                repeat(kept - 1, kept, go(late))
                repeat(kept, head_count, go(lends))

    row = lax.broadcasted_iota(jnp.int32, (8, length), 0)

    def as_rows(a, b):
        a = jnp.sum(jnp.transpose(a), axis=0, keepdims=True)
        b = jnp.sum(jnp.transpose(b), axis=0, keepdims=True)
        return jnp.where(row == 0, a, jnp.where(row == 1, b, 0.0))

    def stats_copy(phase, d, slot):
        return pltpu.make_async_remote_copy(
            src_ref=stats.at[phase, slot],
            dst_ref=stats.at[phase, slot],
            send_sem=stats_send.at[phase, d],
            recv_sem=stats_recv.at[phase, d],
            device_id=peer2(d),
            device_id_type=MESH,
        )

    def stats_go(phase, value):
        stats[phase, me2] = value
        for d in range(1, n2):
            stats_copy(phase, d, me2).start()

    def stats_total(phase):
        for d in range(1, n2):
            stats_copy(phase, d, lax.rem(me2 + n2 - d, n2)).wait_recv()
        return jnp.sum(stats[phase], axis=0)

    loads[0].wait()
    loads[1].wait()

    def square(ref):
        total = jnp.zeros((length, DH), F32)
        for h in range(head_count):
            x = ref[:, h * DH : (h + 1) * DH].astype(F32)
            total = total + x * x
        return total

    stats_go(0, as_rows(square(q), square(k)))
    inner_q[...] = jnp.zeros_like(inner_q)
    inner_k[...] = jnp.zeros_like(inner_k)
    for copy in loads[2:]:
        copy.wait()
    rate_rows = lax.rsqrt(stats_total(0) / features + EPSILON)
    rates[...] = jnp.transpose(rate_rows)
    for nb in range(frames):
        if helped(nb):

            @pl.when(frame == nb)
            def _():
                row_out[...] = rate_rows
                row_copy(nb - 2).start()
                lend(nb, lent // 2, lent)

    def store_grads(cols, q_full, k_full, grad_qn, grad_kn):
        fq = grad_qn * gq[:, cols]
        fk = grad_kn * gk[:, cols]
        flat_q[:, cols] = fq
        flat_k[:, cols] = fk
        inner_q[...] += q_full * fq
        inner_k[...] += k_full * fk
        sums1[me1, 0:1, cols] = jnp.sum(grad_qn * q_full * rates[:, 0:1], axis=0, keepdims=True)
        sums1[me1, 1:2, cols] = jnp.sum(grad_kn * k_full * rates[:, 1:2], axis=0, keepdims=True)

    def head_step(nb, h):
        direct, relayed, _, passes = plan(nb)
        cols = columns(h)
        for j in direct:
            for kv in range(2):
                clean_copy(j, h, kv, passes[0], relay_send.at[0, j]).wait_recv()
                for t, target in enumerate(passes):
                    clean_copy(j, h, kv, target, relay_send.at[t, j]).start()
        rate_q = rates[:, 0:1]
        rate_k = rates[:, 1:2]
        q_full = q[:, cols].astype(F32)
        k_full = k[:, cols].astype(F32)
        gain_q = gq[:, cols]
        gain_k = gk[:, cols]
        qn = (q_full * rate_q * gain_q).astype(BF16)
        kn = (k_full * rate_k * gain_k).astype(BF16)
        val = v[:, cols]
        grad = g[:, cols]
        scores = [dot_nt(qn, kn)]
        grad_probs = [dot_nt(grad, val)]
        for j in relayed:
            for kv in range(2):
                clean_copy(j, h, kv, passes[0], relay_send.at[0, j]).wait_recv()
        for j in range(nb):
            scores.append(dot_nt(qn, cks[j, :, cols]))
            grad_probs.append(dot_nt(grad, cvs[j, :, cols]))
        top = functools.reduce(jnp.maximum, [jnp.max(s, axis=1, keepdims=True) for s in scores])
        expo = [jnp.exp2((s - top) * power) for s in scores]
        total = functools.reduce(jnp.add, [jnp.sum(e, axis=1, keepdims=True) for e in expo])
        summed = dot_nn(expo[0].astype(BF16), val)
        for j in range(nb):
            summed = summed + dot_nn(expo[j + 1].astype(BF16), cvs[j, :, cols])
        inverse = 1.0 / total
        attention = summed * inverse
        att_out[:, cols] = attention.astype(BF16)
        delta = jnp.sum(grad.astype(F32) * attention, axis=1, keepdims=True)
        probs = [e * inverse for e in expo]
        grad_scores = [(p * (d - delta)).astype(BF16) for p, d in zip(probs, grad_probs)]
        grad_qn = dot_nn(grad_scores[0], kn)
        for j in range(nb):
            grad_qn = grad_qn + dot_nn(grad_scores[j + 1], cks[j, :, cols])
        grad_qn = grad_qn * scaling
        grad_kn = dot_tn(grad_scores[0], qn) * scaling
        dv_out[:, cols] = dot_tn(probs[0].astype(BF16), grad).astype(BF16)
        store_grads(cols, q_full, k_full, grad_qn, grad_kn)

    def merged(mine, theirs):
        top1, total1, dot1 = [mine[:, i : i + 1] for i in range(3)]
        top2, total2, dot2 = [theirs[:, i : i + 1] for i in range(3)]
        top = jnp.maximum(top1, top2)
        weight1 = jnp.exp2((top1 - top) * power)
        weight2 = jnp.exp2((top2 - top) * power)
        inverse = 1.0 / (total1 * weight1 + total2 * weight2)
        delta = (dot1 * weight1 + dot2 * weight2) * inverse
        return top, inverse, delta, weight1 * inverse, total2 * weight2 * inverse

    def first_pass(r, qn, grad, keys, values):
        scores = [dot_nt(qn, key) for key in keys]
        top = functools.reduce(jnp.maximum, [jnp.max(s, axis=1, keepdims=True) for s in scores])
        expo = [jnp.exp2((s - top) * power) for s in scores]
        total = functools.reduce(jnp.add, [jnp.sum(e, axis=1, keepdims=True) for e in expo])
        summed = functools.reduce(jnp.add, [dot_nn(e.astype(BF16), val) for e, val in zip(expo, values)])
        near_trip[r, :, 0:1] = top
        near_trip[r, :, 1:2] = total
        near_trip[r, :, 2:3] = jnp.sum(grad.astype(F32) * summed, axis=1, keepdims=True)
        return summed, total

    def second_pass(qn, grad, keys, values, top, inverse, delta):
        probs = [jnp.exp2((dot_nt(qn, key) - top) * power) * inverse for key in keys]
        grad_scores = [(p * (dot_nt(grad, val) - delta)).astype(BF16) for p, val in zip(probs, values)]
        grad_qn = functools.reduce(jnp.add, [dot_nn(s, key) for s, key in zip(grad_scores, keys)]) * scaling
        return probs[0], grad_scores[0], grad_qn

    def trade(target):
        lane = lax.broadcasted_iota(jnp.int32, (length, DH), 1)
        packed = jnp.zeros((length, DH), F32)
        for r in range(lent):
            for i in range(3):
                packed = jnp.where(lane == 3 * r + i, near_trip[r, :, i : i + 1], packed)
        trip_out[...] = jnp.transpose(packed)[: trip_out.shape[0]]
        trip_copy(target).start()

    def traded(target):
        trip_copy(target).wait_recv()
        unpacked = jnp.transpose(trip_in[...])
        for r in range(lent):
            for i in range(3):
                far_trip[r, :, i : i + 1] = unpacked[:, 3 * r + i : 3 * r + i + 1]

    def far_operands(r):
        cols = columns(kept + r)
        q_full = far_q[r].astype(F32)
        rate, gain = far_rates[:, 0:1], gq[:, cols]
        keys = [cks[j, :, cols] for j in range(2)]
        values = [cvs[j, :, cols] for j in range(2)]
        return cols, q_full, rate, gain, (q_full * rate * gain).astype(BF16), far_g[r], keys, values

    def near_operands(nb, r):
        cols = columns(kept + r)
        q_full = q[:, cols].astype(F32)
        k_full = k[:, cols].astype(F32)
        qn = (q_full * rates[:, 0:1] * gq[:, cols]).astype(BF16)
        kn = (k_full * rates[:, 1:2] * gk[:, cols]).astype(BF16)
        keys = [kn] + [cks[j, :, cols] for j in range(2, nb)]
        values = [v[:, cols]] + [cvs[j, :, cols] for j in range(2, nb)]
        return cols, q_full, k_full, qn, g[:, cols], keys, values

    def help_first(nb, r):
        for kind in range(2):
            far_copy(kind, r, nb).wait_recv()
        if nb == 0:
            for kv in range(2):
                clean_copy(1, kept + r, kv, 1, own_send.at[1]).wait_recv()
        _, _, _, _, qn, grad, keys, values = far_operands(r)
        summed, total = first_pass(r, qn, grad, keys, values)
        back_out[1, r] = (summed / total).astype(BF16)

    def help_second(r):
        cols, q_full, rate, gain, qn, grad, keys, values = far_operands(r)
        top, inverse, delta, _, _ = merged(near_trip[r], far_trip[r])
        _, _, grad_qn = second_pass(qn, grad, keys, values, top, inverse, delta)
        back_out[0, r] = grad_qn.astype(BF16)
        far_inner[...] += q_full * (grad_qn * gain)
        sums1[me1, 0:1, cols] += jnp.sum(grad_qn * q_full * rate, axis=0, keepdims=True)

    def near_first(nb, r):
        for j in range(2, nb):
            for kv in range(2):
                clean_copy(j, kept + r, kv, j, own_send.at[1]).wait_recv()
        _, _, _, qn, grad, keys, values = near_operands(nb, r)
        part[r] = first_pass(r, qn, grad, keys, values)[0]

    def near_second(nb, r):
        cols, q_full, k_full, qn, grad, keys, values = near_operands(nb, r)
        top, inverse, delta, near, far = merged(near_trip[r], far_trip[r])
        part[r] = part[r] * near
        far_trip[r, :, 3:4] = far
        probs, grad_scores, grad_qn = second_pass(qn, grad, keys, values, top, inverse, delta)
        grad_kn = dot_tn(grad_scores, qn) * scaling
        dv_out[:, cols] = dot_tn(probs.astype(BF16), grad).astype(BF16)
        store_grads(cols, q_full, k_full, grad_qn, grad_kn)

    for nb in range(frames):

        @pl.when(frame == nb)
        def _():
            if helps(nb):
                repeat(0, head_count, functools.partial(head_step, nb))
                row_copy(nb + 2).wait_recv()
                far_rates[...] = jnp.transpose(row_in[...])
                repeat(0, lent, functools.partial(help_first, nb))
                trade(nb + 2)
                send_own(nb, kept - 1, [(0, nb + 2)])
                far_inner[...] = jnp.zeros_like(far_inner)
                traded(nb + 2)
                repeat(0, lent, help_second)
                row_out[...] = as_rows(far_inner[...], jnp.zeros_like(far_inner))
                row_copy(nb + 2).start()
                stats_go(1, as_rows(inner_q[...], inner_k[...]))
            elif helped(nb):
                repeat(0, lent, functools.partial(near_first, nb))
                trade(nb - 2)
                repeat(0, kept - 1, functools.partial(head_step, nb))
                traded(nb - 2)
                repeat(0, lent, functools.partial(near_second, nb))
                repeat(kept - 1, kept, functools.partial(head_step, nb))
                row_copy(nb - 2).wait_recv()
                stats_go(1, as_rows(inner_q[...], inner_k[...]) + row_in[...])
            else:
                repeat(0, head_count, functools.partial(head_step, nb))
                stats_go(1, as_rows(inner_q[...], inner_k[...]))

    def s1_copy(d, slot):
        return pltpu.make_async_remote_copy(
            src_ref=sums1.at[slot],
            dst_ref=sums1.at[slot],
            send_sem=s1_send.at[d],
            recv_sem=s1_recv.at[d],
            device_id=peer1(d),
            device_id_type=MESH,
        )

    def s2_copy(d, slot):
        return pltpu.make_async_remote_copy(
            src_ref=sums2.at[slot],
            dst_ref=sums2.at[slot],
            send_sem=s2_send.at[d],
            recv_sem=s2_recv.at[d],
            device_id=peer2(d),
            device_id_type=MESH,
        )

    def s1_go(d, _):
        s1_copy(d, me1).start()
        return 0

    lax.fori_loop(1, n1, s1_go, 0)
    for nb in range(frames):
        if helps(nb):

            @pl.when(frame == nb)
            def _():
                for kind in range(2):
                    repeat(0, lent, lambda r: back_copy(kind, r, nb + 2).start())

    inners = jnp.transpose(stats_total(1))
    rate_q = rates[:, 0:1]
    rate_k = rates[:, 1:2]
    cube_q = rate_q * rate_q * rate_q * inners[:, 0:1] / features
    cube_k = rate_k * rate_k * rate_k * inners[:, 1:2] / features

    def s1_land(d, _):
        s1_copy(d, lax.rem(me1 + n1 - d, n1)).wait_recv()
        return 0

    lax.fori_loop(1, n1, s1_land, 0)
    sums2[me2] = jnp.sum(sums1[...], axis=0)
    for d in range(1, n2):
        s2_copy(d, me2).start()

    def finish(h, _):
        cols = columns(h)
        dq_out[:, cols] = (rate_q * flat_q[:, cols] - q[:, cols].astype(F32) * cube_q).astype(BF16)
        dk_out[:, cols] = (rate_k * flat_k[:, cols] - k[:, cols].astype(F32) * cube_k).astype(BF16)
        return 0

    lax.fori_loop(0, kept, finish, 0)
    for nb in range(frames):
        if helped(nb):

            @pl.when(frame == nb)
            def _():
                def add(r):
                    cols = columns(kept + r)
                    back_copy(0, r, nb - 2).wait_recv()
                    flat_q[:, cols] += back_in[0, r].astype(F32) * gq[:, cols]

                repeat(0, lent, add)

    lax.fori_loop(kept, head_count, finish, 0)
    for d in range(1, n2):
        s2_copy(d, lax.rem(me2 + n2 - d, n2)).wait_recv()
    for p in range(n2):
        gain_q_out[:, p * width : (p + 1) * width] = sums2[p, 0:1, :]
        gain_k_out[:, p * width : (p + 1) * width] = sums2[p, 1:2, :]

    for nb in range(frames):
        if helped(nb):

            @pl.when(frame == nb)
            def _():
                def join(r):
                    back_copy(1, r, nb - 2).wait_recv()
                    far = back_in[1, r].astype(F32) * far_trip[r, :, 3:4]
                    att_out[:, columns(kept + r)] = (part[r] + far).astype(BF16)

                repeat(0, lent, join)

    for d in range(1, n2):
        stats_copy(0, d, me2).wait_send()
        stats_copy(1, d, me2).wait_send()
        s2_copy(d, me2).wait_send()

    def s1_gone(d, _):
        s1_copy(d, me1).wait_send()
        return 0

    lax.fori_loop(1, n1, s1_gone, 0)
    for nb in range(frames):
        direct, _, _, passes = plan(nb)
        full, _, lends = own_lists(nb)

        @pl.when(frame == nb)
        def _():
            def gone(targets, relays):
                def step(h):
                    for kv in range(2):
                        for t, target in targets:
                            clean_copy(nb, h, kv, target, own_send.at[t]).wait_send()
                        for j in relays:
                            for t, target in enumerate(passes):
                                clean_copy(j, h, kv, target, relay_send.at[t, j]).wait_send()

                return step

            repeat(0, kept, gone(full, direct))
            repeat(kept, head_count, gone(lends, []))
            if helps(nb) or helped(nb):
                other = nb + 2 if helps(nb) else nb - 2
                trip_copy(other).wait_send()
                row_copy(other).wait_send()
                copy = back_copy if helps(nb) else far_copy
                for kind in range(2):
                    repeat(0, lent, lambda r: copy(kind, r, other).wait_send())


def write_out(*refs):
    sem = refs[12]
    copies = [pltpu.make_async_copy(refs[i], refs[6 + i], sem.at[i]) for i in range(6)]
    for copy in copies:
        copy.start()
    for copy in copies:
        copy.wait()


def on_device(queries, noisy_keys, noisy_values, clean_keys, clean_values, gain_query, gain_key, out_grad):
    length, width = queries.shape
    features = gain_query.shape[0]
    frames = lax.axis_size("frame")
    fsdp = lax.axis_size("fsdp")
    heads_axis = lax.axis_size("head")
    head_count = width // DH
    n1 = frames * (fsdp // 2)
    n2 = 2 * heads_axis
    block = pltpu.VMEM((length, width), BF16)
    gains = pltpu.VMEM((1, features), F32)
    anywhere = pl.BlockSpec(memory_space=pl.ANY)
    vmem = pl.BlockSpec(memory_space=pltpu.VMEM)
    dma = pltpu.SemaphoreType.DMA
    earlier = max(frames - 1, 1)
    kept = 4 * 2 * length * width + 2 * 4 * features
    lent = head_count * 2 // 5 if frames == 4 else 0
    held = max(lent, 1)
    trip_rows = -(-3 * held // 8) * 8
    outs = pl.pallas_call(
        functools.partial(kernel, frames, fsdp, heads_axis, width, features, lent),
        out_shape=(block, block, block, block, gains, gains),
        in_specs=[anywhere] * 8,
        out_specs=[vmem] * 6,
        scratch_shapes=[
            pltpu.VMEM((length, width), BF16),
            pltpu.VMEM((length, width), BF16),
            pltpu.VMEM((length, width), BF16),
            pltpu.VMEM((length, width), BF16),
            pltpu.VMEM((1, width), F32),
            pltpu.VMEM((1, width), F32),
            pltpu.VMEM((frames, length, width), BF16),
            pltpu.VMEM((frames, length, width), BF16),
            pltpu.VMEM((length, width), F32),
            pltpu.VMEM((length, width), F32),
            pltpu.VMEM((length, DH), F32),
            pltpu.VMEM((length, DH), F32),
            pltpu.VMEM((length, 8), F32),
            pltpu.VMEM((2, n2, 8, length), F32),
            pltpu.VMEM((n1, 2, width), F32),
            pltpu.VMEM((n2, 2, width), F32),
            pltpu.VMEM((held, length, DH), BF16),
            pltpu.VMEM((held, length, DH), BF16),
            pltpu.VMEM((length, 8), F32),
            pltpu.VMEM((length, DH), F32),
            pltpu.VMEM((held, length, DH), F32),
            pltpu.VMEM((2, held, length, DH), BF16),
            pltpu.VMEM((2, held, length, DH), BF16),
            pltpu.VMEM((held, length, 8), F32),
            pltpu.VMEM((held, length, 8), F32),
            pltpu.VMEM((trip_rows, length), F32),
            pltpu.VMEM((trip_rows, length), F32),
            pltpu.VMEM((8, length), F32),
            pltpu.VMEM((8, length), F32),
            dma((6,)),
            dma((2, head_count, 2)),
            dma((2, earlier, head_count, 2)),
            dma((frames, head_count, 2)),
            dma((2, n2)),
            dma((2, n2)),
            dma((n1,)),
            dma((n1,)),
            dma((n2,)),
            dma((n2,)),
            dma((head_count, 2)),
            dma((2, held)),
            dma((2, held)),
            dma((2, held)),
            dma((2, held)),
            dma((1,)),
            dma((1,)),
            dma((1,)),
            dma((1,)),
        ],
        compiler_params=pltpu.CompilerParams(
            collective_id=0, has_side_effects=True, vmem_limit_bytes=VMEM_BYTES - kept - 4096
        ),
        name="attention",
    )(
        queries, noisy_keys, noisy_values, clean_keys, clean_values,
        gain_query.reshape(1, features), gain_key.reshape(1, features), out_grad,
    )
    outs = pl.pallas_call(
        write_out,
        out_shape=tuple(jax.ShapeDtypeStruct(out.shape, out.dtype) for out in outs),
        in_specs=[anywhere] * 6,
        out_specs=[anywhere] * 6,
        scratch_shapes=[dma((6,))],
        compiler_params=pltpu.CompilerParams(vmem_limit_bytes=8 * 1024 * 1024),
        name="write_out",
    )(*outs)
    return (*outs[:4], outs[4].reshape(features), outs[5].reshape(features))


def solution(mesh):
    tokens = P("frame", ("fsdp", "head"))
    return jax.shard_map(
        on_device,
        mesh=mesh,
        in_specs=(tokens, tokens, tokens, tokens, tokens, P(), P(), tokens),
        out_specs=(tokens, tokens, tokens, tokens, P(), P()),
        check_vma=False,
    )
```

```python
import functools
import math

import jax
import jax.numpy as jnp
from jax import lax
from jax.experimental import pallas as pl
from jax.experimental.pallas import tpu as pltpu
from jax.sharding import PartitionSpec as P

DH = 128
EPSILON = 1e-06
MESH = pl.DeviceIdType.MESH
VMEM_BYTES = 67043328
F32 = jnp.float32
BF16 = jnp.bfloat16


def dot_nt(a, b):
    return lax.dot_general(a, b, (((1,), (1,)), ((), ())), preferred_element_type=F32)


def dot_nn(a, b):
    return lax.dot_general(a, b, (((1,), (0,)), ((), ())), preferred_element_type=F32)


def dot_tn(a, b):
    return lax.dot_general(a, b, (((0,), (0,)), ((), ())), preferred_element_type=F32)


def kernel(
    frames, fsdp, heads_axis, width, features, lent,
    q_hbm, k_hbm, v_hbm, ck_hbm, cv_hbm, gq_hbm, gk_hbm, g_hbm,
    att_out, dq_out, dk_out, dv_out, gain_q_out, gain_k_out,
    tokens, gains, clean, flat_q, flat_k, inner_q, inner_k, rates,
    stats, sums1, sums2, far, far_rates, far_inner, far_sums, part, back_out, back_in,
    near_trip, far_trip, trip_out, trip_in, row_out, row_in,
    load_sem, own_send, relay_send, direct_recv, relay_recv, partner_recv, stats_send, stats_recv, sum_send, sum_recv,
    far_send, far_recv, back_send, grad_recv, att_recv, row_send, row_recv,
):
    q, k, v, g = [tokens.at[i] for i in range(4)]
    gq, gk = gains.at[0], gains.at[1]
    length = tokens.shape[1]
    head_count = width // DH
    kept = head_count - lent
    videos = fsdp // 2
    scaling = 1.0 / math.sqrt(DH)
    power = scaling * math.log2(math.e)
    frame = lax.axis_index("frame")
    fs = lax.axis_index("fsdp")
    half = fs // videos
    video = lax.rem(fs, videos)
    me1 = frame * videos + video
    n1 = frames * videos
    me2 = half * heads_axis + lax.axis_index("head")
    n2 = 2 * heads_axis

    def peer1(distance):
        p = lax.rem(me1 + distance, n1)
        return {"frame": p // videos, "fsdp": half * videos + lax.rem(p, videos)}

    def peer2(distance):
        p = lax.rem(me2 + distance, n2)
        return {"fsdp": (p // heads_axis) * videos + video, "head": lax.rem(p, heads_axis)}

    def columns(h):
        return pl.ds(pl.multiple_of(h * DH, DH), DH)

    def repeat(first, last, step):
        def body(i, _):
            step(i)
            return 0

        lax.fori_loop(first, last, body, 0)

    def arrive(ref, sem):
        pltpu.make_async_copy(ref, ref, sem).wait()

    for nb in range(frames - 1):

        @pl.when(frame == nb)
        def _():
            for kv, src in enumerate((ck_hbm, cv_hbm)):
                pltpu.make_async_copy(src, clean.at[nb, kv], load_sem.at[3]).start()

    barrier = pltpu.get_barrier_semaphore()

    def greet(d, _):
        pl.semaphore_signal(barrier, inc=1, device_id=peer1(d), device_id_type=MESH)
        return 0

    lax.fori_loop(1, n1, greet, 0)
    for d in range(1, n2):
        pl.semaphore_signal(barrier, inc=1, device_id=peer2(d), device_id_type=MESH)
    start = pl.multiple_of(me2 * width, DH)
    for src, dst, i in (
        (q_hbm, q, 0),
        (k_hbm, k, 0),
        (gq_hbm.at[:, pl.ds(start, width)], gq, 1),
        (gk_hbm.at[:, pl.ds(start, width)], gk, 1),
        (v_hbm, v, 2),
        (g_hbm, g, 2),
    ):
        pltpu.make_async_copy(src, dst, load_sem.at[i]).start()
    pl.semaphore_wait(barrier, n1 - 1 + n2 - 1)

    def frame_copy(src, dst, send, recv, target):
        return pltpu.make_async_remote_copy(
            src_ref=src,
            dst_ref=dst,
            send_sem=send,
            recv_sem=recv,
            device_id={"frame": jnp.int32(target)},
            device_id_type=MESH,
        )

    def direct_copy(j, h, target, send):
        land = clean.at[j, :, :, columns(h)]
        return frame_copy(land, land, send, direct_recv.at[j // 2, h], target)

    def relay_copy(j, h, target, send):
        land = clean.at[j, :, :, columns(h)]
        return frame_copy(land, land, send, relay_recv.at[j // 2, h], target)

    def partner_copy(j):
        land = clean.at[j] if j % 2 == 0 else clean.at[j, :, :, pl.ds(kept * DH, lent * DH)]
        return frame_copy(land, land, own_send.at[1], partner_recv.at[0], 2 * (j // 2) + 1 - j % 2)

    def kept_heads(j, sem):
        land = clean.at[j, :, :, pl.ds(0, kept * DH)]
        return frame_copy(land, land, sem, partner_recv.at[0], (j + 1) % frames)

    def plan(nb):
        pair, side = nb // 2, nb % 2
        partner, further = 2 * pair + 1 - side, nb + 2
        direct = [2 * c + side for c in range(pair)]
        relayed = [2 * c + 1 - side for c in range(pair)]
        return direct, relayed, partner, further if further < frames else None

    def helps(nb):
        return lent > 0 and nb < 2

    def helped(nb):
        return lent > 0 and nb >= 2

    def has_partner_copy(nb):
        return nb % 2 == 0 or helps(nb)

    def send_own(nb, first, last):
        further = plan(nb)[3]
        repeat(first, last, lambda h: direct_copy(nb, h, further, own_send.at[0]).start())

    def far_copy(kind, r, target):
        src = (q_hbm, g_hbm)[kind].at[:, columns(kept + r)]
        return frame_copy(src, far.at[r, kind], far_send.at[0], far_recv.at[r], target)

    def back_copy(kind, r, target):
        recv = grad_recv.at[0] if kind == 0 else att_recv.at[r]
        return frame_copy(back_out.at[kind, r], back_in.at[kind, r], back_send.at[0], recv, target)

    def trip_copy(target):
        return frame_copy(trip_out, trip_in, row_send.at[1], row_recv.at[1], target)

    def row_copy(target):
        return frame_copy(row_out, row_in, row_send.at[0], row_recv.at[0], target)

    def lend(nb, first, last):
        def go(r):
            for kind in range(2):
                far_copy(kind, r, nb - 2).start()

        repeat(first, last, go)

    for nb in range(frames):

        @pl.when(frame == nb)
        def _():
            if helped(nb):
                lend(nb, 0, lent // 2)
            if nb < frames - 1:
                arrive(clean.at[nb], load_sem.at[3])
            if plan(nb)[3] is not None:
                send_own(nb, 0, kept - 1 if helps(nb) else kept)
            if has_partner_copy(nb):
                partner_copy(nb).start()

    row = lax.broadcasted_iota(jnp.int32, (8, length), 0)

    def as_rows(a, b):
        a = jnp.sum(jnp.transpose(a), axis=0, keepdims=True)
        b = jnp.sum(jnp.transpose(b), axis=0, keepdims=True)
        return jnp.where(row == 0, a, jnp.where(row == 1, b, 0.0))

    def stats_copy(phase, d, part):
        return pltpu.make_async_remote_copy(
            src_ref=part,
            dst_ref=part,
            send_sem=stats_send.at[phase],
            recv_sem=stats_recv.at[phase],
            device_id=peer2(d),
            device_id_type=MESH,
        )

    def all_stats(phase):
        return stats_copy(phase, 1, stats.at[phase, pl.ds(0, n2 - 1)])

    def stats_go(phase, value):
        stats[phase, me2] = value
        for d in range(1, n2):
            stats_copy(phase, d, stats.at[phase, me2]).start()

    def stats_total(phase):
        all_stats(phase).wait_recv()
        return jnp.sum(stats[phase], axis=0)

    arrive(tokens.at[pl.ds(0, 2)], load_sem.at[0])

    def square(ref):
        total = jnp.zeros((length, DH), F32)
        for h in range(head_count):
            x = ref[:, h * DH : (h + 1) * DH].astype(F32)
            total = total + x * x
        return total

    stats_go(0, as_rows(square(q), square(k)))
    inner_q[...] = jnp.zeros_like(inner_q)
    inner_k[...] = jnp.zeros_like(inner_k)
    arrive(gains, load_sem.at[1])
    arrive(tokens.at[pl.ds(2, 2)], load_sem.at[2])
    rate_rows = lax.rsqrt(stats_total(0) / features + EPSILON)
    rates[...] = jnp.transpose(rate_rows)
    for nb in range(frames):
        if helped(nb):

            @pl.when(frame == nb)
            def _():
                row_out[...] = rate_rows
                row_copy(nb - 2).start()
                lend(nb, lent // 2, lent)

    def store_grads(cols, q_full, k_full, grad_qn, grad_kn):
        fq = grad_qn * gq[:, cols]
        fk = grad_kn * gk[:, cols]
        flat_q[:, cols] = fq
        flat_k[:, cols] = fk
        inner_q[...] += q_full * fq
        inner_k[...] += k_full * fk
        sums1[me1, 0:1, cols] = jnp.sum(grad_qn * q_full * rates[:, 0:1], axis=0, keepdims=True)
        sums1[me1, 1:2, cols] = jnp.sum(grad_kn * k_full * rates[:, 1:2], axis=0, keepdims=True)

    def head_step(nb, h):
        direct, relayed, partner, further = plan(nb)
        cols = columns(h)
        for j in direct:
            direct_copy(j, h, partner, relay_send.at[0, j // 2]).wait_recv()
            relay_copy(j, h, partner, relay_send.at[0, j // 2]).start()
            if further is not None:
                direct_copy(j, h, further, relay_send.at[1, j // 2]).start()
        rate_q = rates[:, 0:1]
        rate_k = rates[:, 1:2]
        q_full = q[:, cols].astype(F32)
        k_full = k[:, cols].astype(F32)
        gain_q = gq[:, cols]
        gain_k = gk[:, cols]
        qn = (q_full * rate_q * gain_q).astype(BF16)
        kn = (k_full * rate_k * gain_k).astype(BF16)
        val = v[:, cols]
        grad = g[:, cols]
        scores = [dot_nt(qn, kn)]
        grad_probs = [dot_nt(grad, val)]
        for j in relayed:
            relay_copy(j, h, partner, relay_send.at[0, j // 2]).wait_recv()
        for j in range(nb):
            scores.append(dot_nt(qn, clean[j, 0, :, cols]))
            grad_probs.append(dot_nt(grad, clean[j, 1, :, cols]))
        top = functools.reduce(jnp.maximum, [jnp.max(s, axis=1, keepdims=True) for s in scores])
        expo = [jnp.exp2((s - top) * power) for s in scores]
        total = functools.reduce(jnp.add, [jnp.sum(e, axis=1, keepdims=True) for e in expo])
        summed = dot_nn(expo[0].astype(BF16), val)
        for j in range(nb):
            summed = summed + dot_nn(expo[j + 1].astype(BF16), clean[j, 1, :, cols])
        inverse = 1.0 / total
        attention = summed * inverse
        att_out[:, cols] = attention.astype(BF16)
        delta = jnp.sum(grad.astype(F32) * attention, axis=1, keepdims=True)
        probs = [e * inverse for e in expo]
        grad_scores = [(p * (d - delta)).astype(BF16) for p, d in zip(probs, grad_probs)]
        grad_qn = dot_nn(grad_scores[0], kn)
        for j in range(nb):
            grad_qn = grad_qn + dot_nn(grad_scores[j + 1], clean[j, 0, :, cols])
        grad_qn = grad_qn * scaling
        grad_kn = dot_tn(grad_scores[0], qn) * scaling
        dv_out[:, cols] = dot_tn(probs[0].astype(BF16), grad).astype(BF16)
        store_grads(cols, q_full, k_full, grad_qn, grad_kn)

    def merged(mine, theirs):
        top1, total1, dot1 = [mine[:, i : i + 1] for i in range(3)]
        top2, total2, dot2 = [theirs[:, i : i + 1] for i in range(3)]
        top = jnp.maximum(top1, top2)
        weight1 = jnp.exp2((top1 - top) * power)
        weight2 = jnp.exp2((top2 - top) * power)
        inverse = 1.0 / (total1 * weight1 + total2 * weight2)
        delta = (dot1 * weight1 + dot2 * weight2) * inverse
        return top, inverse, delta, weight1 * inverse, total2 * weight2 * inverse

    def first_pass(r, qn, grad, keys, values):
        scores = [dot_nt(qn, key) for key in keys]
        top = functools.reduce(jnp.maximum, [jnp.max(s, axis=1, keepdims=True) for s in scores])
        expo = [jnp.exp2((s - top) * power) for s in scores]
        total = functools.reduce(jnp.add, [jnp.sum(e, axis=1, keepdims=True) for e in expo])
        summed = functools.reduce(jnp.add, [dot_nn(e.astype(BF16), val) for e, val in zip(expo, values)])
        near_trip[r, :, 0:1] = top
        near_trip[r, :, 1:2] = total
        near_trip[r, :, 2:3] = jnp.sum(grad.astype(F32) * summed, axis=1, keepdims=True)
        return summed, total

    def second_pass(qn, grad, keys, values, top, inverse, delta):
        probs = [jnp.exp2((dot_nt(qn, key) - top) * power) * inverse for key in keys]
        grad_scores = [(p * (dot_nt(grad, val) - delta)).astype(BF16) for p, val in zip(probs, values)]
        grad_qn = functools.reduce(jnp.add, [dot_nn(s, key) for s, key in zip(grad_scores, keys)]) * scaling
        return probs[0], grad_scores[0], grad_qn

    def trade(target):
        lane = lax.broadcasted_iota(jnp.int32, (length, DH), 1)
        packed = jnp.zeros((length, DH), F32)
        for r in range(lent):
            for i in range(3):
                packed = jnp.where(lane == 3 * r + i, near_trip[r, :, i : i + 1], packed)
        trip_out[...] = jnp.transpose(packed)[: trip_out.shape[0]]
        trip_copy(target).start()

    def traded(target):
        trip_copy(target).wait_recv()
        unpacked = jnp.transpose(trip_in[...])
        for r in range(lent):
            for i in range(3):
                far_trip[r, :, i : i + 1] = unpacked[:, 3 * r + i : 3 * r + i + 1]

    def far_operands(r):
        cols = columns(kept + r)
        q_full = far[r, 0].astype(F32)
        rate, gain = far_rates[:, 0:1], gq[:, cols]
        keys = [clean[j, 0, :, cols] for j in range(2)]
        values = [clean[j, 1, :, cols] for j in range(2)]
        return cols, q_full, rate, gain, (q_full * rate * gain).astype(BF16), far[r, 1], keys, values

    def near_operands(nb, r):
        cols = columns(kept + r)
        q_full = q[:, cols].astype(F32)
        k_full = k[:, cols].astype(F32)
        qn = (q_full * rates[:, 0:1] * gq[:, cols]).astype(BF16)
        kn = (k_full * rates[:, 1:2] * gk[:, cols]).astype(BF16)
        keys = [kn] + [clean[j, 0, :, cols] for j in range(2, nb)]
        values = [v[:, cols]] + [clean[j, 1, :, cols] for j in range(2, nb)]
        return cols, q_full, k_full, qn, g[:, cols], keys, values

    def help_first(nb, r):
        frame_copy(far.at[r], far.at[r], far_send.at[0], far_recv.at[r], nb + 2).wait_recv()
        _, _, _, _, qn, grad, keys, values = far_operands(r)
        summed, total = first_pass(r, qn, grad, keys, values)
        back_out[1, r] = (summed / total).astype(BF16)

    def help_second(r):
        cols, q_full, rate, gain, qn, grad, keys, values = far_operands(r)
        top, inverse, delta, _, _ = merged(near_trip[r], far_trip[r])
        _, _, grad_qn = second_pass(qn, grad, keys, values, top, inverse, delta)
        back_out[0, r] = grad_qn.astype(BF16)
        far_inner[...] += q_full * (grad_qn * gain)
        far_sums[pl.ds(r, 1), :] = jnp.sum(grad_qn * q_full * rate, axis=0, keepdims=True)

    def near_first(nb, r):
        _, _, _, qn, grad, keys, values = near_operands(nb, r)
        part[r] = first_pass(r, qn, grad, keys, values)[0]

    def near_second(nb, r):
        cols, q_full, k_full, qn, grad, keys, values = near_operands(nb, r)
        top, inverse, delta, near, far = merged(near_trip[r], far_trip[r])
        part[r] = part[r] * near
        far_trip[r, :, 3:4] = far
        probs, grad_scores, grad_qn = second_pass(qn, grad, keys, values, top, inverse, delta)
        grad_kn = dot_tn(grad_scores, qn) * scaling
        dv_out[:, cols] = dot_tn(probs.astype(BF16), grad).astype(BF16)
        store_grads(cols, q_full, k_full, grad_qn, grad_kn)

    for nb in range(frames):

        @pl.when(frame == nb)
        def _():
            own = functools.partial(head_step, nb)
            if nb % 2 == 1:
                partner_copy(nb - 1).wait_recv()
            if helps(nb):
                first, middle = head_count * 3 // 10, head_count // 2
                repeat(0, first, own)
                if nb == 0:
                    partner_copy(1).wait_recv()
                row_copy(nb + 2).wait_recv()
                far_rates[...] = jnp.transpose(row_in[...])
                repeat(0, lent // 2, functools.partial(help_first, nb))
                repeat(first, middle, own)
                repeat(lent // 2, lent, functools.partial(help_first, nb))
                trade(nb + 2)
                send_own(nb, kept - 1, kept)
                far_inner[...] = jnp.zeros_like(far_inner)
                traded(nb + 2)
                repeat(0, lent, help_second)
                row_out[...] = as_rows(far_inner[...], jnp.zeros_like(far_inner))
                row_copy(nb + 2).start()
                repeat(0, lent, lambda r: back_copy(0, r, nb + 2).start())
                repeat(middle, head_count, own)
                for r in range(lent):
                    cols = columns(kept + r)
                    sums1[me1, 0:1, cols] += far_sums[r : r + 1, :]
                stats_go(1, as_rows(inner_q[...], inner_k[...]))
            elif helped(nb):
                repeat(0, lent, functools.partial(near_first, nb))
                trade(nb - 2)
                repeat(0, kept - 1, own)
                traded(nb - 2)
                repeat(0, lent, functools.partial(near_second, nb))
                repeat(kept - 1, kept, own)
                row_copy(nb - 2).wait_recv()
                stats_go(1, as_rows(inner_q[...], inner_k[...]) + row_in[...])
            else:
                repeat(0, head_count, own)
                stats_go(1, as_rows(inner_q[...], inner_k[...]))

    def s1_copy(d, part):
        return pltpu.make_async_remote_copy(
            src_ref=part,
            dst_ref=part,
            send_sem=sum_send.at[0],
            recv_sem=sum_recv.at[0],
            device_id=peer1(d),
            device_id_type=MESH,
        )

    def s2_copy(d, part):
        return pltpu.make_async_remote_copy(
            src_ref=part,
            dst_ref=part,
            send_sem=sum_send.at[1],
            recv_sem=sum_recv.at[1],
            device_id=peer2(d),
            device_id_type=MESH,
        )

    all_s1 = s1_copy(1, sums1.at[pl.ds(0, n1 - 1)])
    all_s2 = s2_copy(1, sums2.at[pl.ds(0, n2 - 1)])
    repeat(1, n1, lambda d: s1_copy(d, sums1.at[me1]).start())
    for nb in range(frames):
        if helps(nb):

            @pl.when(frame == nb)
            def _():
                repeat(0, lent, lambda r: back_copy(1, r, nb + 2).start())

    inners = jnp.transpose(stats_total(1))
    rate_q = rates[:, 0:1]
    rate_k = rates[:, 1:2]
    cube_q = rate_q * rate_q * rate_q * inners[:, 0:1] / features
    cube_k = rate_k * rate_k * rate_k * inners[:, 1:2] / features

    all_s1.wait_recv()
    sums2[me2] = jnp.sum(sums1[...], axis=0)
    for d in range(1, n2):
        s2_copy(d, sums2.at[me2]).start()

    def finish(h, _):
        cols = columns(h)
        dq_out[:, cols] = (rate_q * flat_q[:, cols] - q[:, cols].astype(F32) * cube_q).astype(BF16)
        dk_out[:, cols] = (rate_k * flat_k[:, cols] - k[:, cols].astype(F32) * cube_k).astype(BF16)
        return 0

    lax.fori_loop(0, kept, finish, 0)
    for nb in range(frames):
        if helped(nb):

            @pl.when(frame == nb)
            def _():
                grads = back_in.at[0]
                frame_copy(grads, grads, back_send.at[0], grad_recv.at[0], nb - 2).wait_recv()

                def add(r):
                    cols = columns(kept + r)
                    flat_q[:, cols] += back_in[0, r].astype(F32) * gq[:, cols]

                repeat(0, lent, add)

    lax.fori_loop(kept, head_count, finish, 0)
    all_s2.wait_recv()
    for p in range(n2):
        gain_q_out[:, p * width : (p + 1) * width] = sums2[p, 0:1, :]
        gain_k_out[:, p * width : (p + 1) * width] = sums2[p, 1:2, :]

    for nb in range(frames):
        if helped(nb):

            @pl.when(frame == nb)
            def _():
                def join(r):
                    back_copy(1, r, nb - 2).wait_recv()
                    far = back_in[1, r].astype(F32) * far_trip[r, :, 3:4]
                    att_out[:, columns(kept + r)] = (part[r] + far).astype(BF16)

                repeat(0, lent, join)

    all_stats(0).wait_send()
    all_stats(1).wait_send()
    all_s1.wait_send()
    all_s2.wait_send()
    for nb in range(frames):
        direct, _, _, further = plan(nb)

        @pl.when(frame == nb)
        def _():
            if further is not None:
                kept_heads(nb, own_send.at[0]).wait_send()
            if has_partner_copy(nb):
                partner_copy(nb).wait_send()
            for j in direct:
                for t in range(1 if further is None else 2):
                    kept_heads(j, relay_send.at[t, j // 2]).wait_send()
            if helps(nb) or helped(nb):
                other = nb + 2 if helps(nb) else nb - 2
                trip_copy(other).wait_send()
                row_copy(other).wait_send()
            if helps(nb):
                frame_copy(back_out, back_in, back_send.at[0], grad_recv.at[0], nb + 2).wait_send()
            if helped(nb):
                frame_copy(far, far, far_send.at[0], far_recv.at[0], nb - 2).wait_send()


def write_out(*refs):
    sem = refs[12]
    copies = [pltpu.make_async_copy(refs[i], refs[6 + i], sem.at[i]) for i in range(6)]
    for copy in copies:
        copy.start()
    for copy in copies:
        copy.wait()


def on_device(queries, noisy_keys, noisy_values, clean_keys, clean_values, gain_query, gain_key, out_grad):
    length, width = queries.shape
    features = gain_query.shape[0]
    frames = lax.axis_size("frame")
    fsdp = lax.axis_size("fsdp")
    heads_axis = lax.axis_size("head")
    head_count = width // DH
    n1 = frames * (fsdp // 2)
    n2 = 2 * heads_axis
    block = pltpu.VMEM((length, width), BF16)
    gains = pltpu.VMEM((1, features), F32)
    anywhere = pl.BlockSpec(memory_space=pl.ANY)
    vmem = pl.BlockSpec(memory_space=pltpu.VMEM)
    dma = pltpu.SemaphoreType.DMA
    chips = max(frames // 2 - 1, 1)
    kept = 4 * 2 * length * width + 2 * 4 * features
    lent = head_count * 2 // 5 if frames == 4 else 0
    held = max(lent, 1)
    kept_count = head_count - lent
    trip_rows = -(-3 * held // 8) * 8
    outs = pl.pallas_call(
        functools.partial(kernel, frames, fsdp, heads_axis, width, features, lent),
        out_shape=(block, block, block, block, gains, gains),
        in_specs=[anywhere] * 8,
        out_specs=[vmem] * 6,
        scratch_shapes=[
            pltpu.VMEM((4, length, width), BF16),
            pltpu.VMEM((2, 1, width), F32),
            pltpu.VMEM((frames, 2, length, width), BF16),
            pltpu.VMEM((length, width), F32),
            pltpu.VMEM((length, width), F32),
            pltpu.VMEM((length, DH), F32),
            pltpu.VMEM((length, DH), F32),
            pltpu.VMEM((length, 8), F32),
            pltpu.VMEM((2, n2, 8, length), F32),
            pltpu.VMEM((n1, 2, width), F32),
            pltpu.VMEM((n2, 2, width), F32),
            pltpu.VMEM((held, 2, length, DH), BF16),
            pltpu.VMEM((length, 8), F32),
            pltpu.VMEM((length, DH), F32),
            pltpu.VMEM((-(-held // 8) * 8, DH), F32),
            pltpu.VMEM((held, length, DH), F32),
            pltpu.VMEM((2, held, length, DH), BF16),
            pltpu.VMEM((2, held, length, DH), BF16),
            pltpu.VMEM((held, length, 8), F32),
            pltpu.VMEM((held, length, 8), F32),
            pltpu.VMEM((trip_rows, length), F32),
            pltpu.VMEM((trip_rows, length), F32),
            pltpu.VMEM((8, length), F32),
            pltpu.VMEM((8, length), F32),
            dma((4,)),
            dma((2,)),
            dma((2, chips)),
            dma((chips, kept_count)),
            dma((chips, kept_count)),
            dma((1,)),
            dma((2,)),
            dma((2,)),
            dma((2,)),
            dma((2,)),
            dma((1,)),
            dma((held,)),
            dma((1,)),
            dma((1,)),
            dma((held,)),
            dma((2,)),
            dma((2,)),
        ],
        compiler_params=pltpu.CompilerParams(
            collective_id=0, has_side_effects=True, vmem_limit_bytes=VMEM_BYTES - kept - 4096
        ),
        name="attention",
    )(
        queries, noisy_keys, noisy_values, clean_keys, clean_values,
        gain_query.reshape(1, features), gain_key.reshape(1, features), out_grad,
    )
    outs = pl.pallas_call(
        write_out,
        out_shape=tuple(jax.ShapeDtypeStruct(out.shape, out.dtype) for out in outs),
        in_specs=[anywhere] * 6,
        out_specs=[anywhere] * 6,
        scratch_shapes=[dma((6,))],
        compiler_params=pltpu.CompilerParams(vmem_limit_bytes=8 * 1024 * 1024),
        name="write_out",
    )(*outs)
    return (*outs[:4], outs[4].reshape(features), outs[5].reshape(features))


def solution(mesh):
    tokens = P("frame", ("fsdp", "head"))
    return jax.shard_map(
        on_device,
        mesh=mesh,
        in_specs=(tokens, tokens, tokens, tokens, tokens, P(), P(), tokens),
        out_specs=(tokens, tokens, tokens, tokens, P(), P()),
        check_vma=False,
    )
```

```python
import functools
import math

import jax
import jax.numpy as jnp
from jax import lax
from jax.experimental import pallas as pl
from jax.experimental.pallas import tpu as pltpu
from jax.sharding import PartitionSpec as P

DH = 128
EPSILON = 1e-06
MESH = pl.DeviceIdType.MESH
VMEM_BYTES = 67043328
F32 = jnp.float32
BF16 = jnp.bfloat16


def dot_nt(a, b):
    return lax.dot_general(a, b, (((1,), (1,)), ((), ())), preferred_element_type=F32)


def dot_nn(a, b):
    return lax.dot_general(a, b, (((1,), (0,)), ((), ())), preferred_element_type=F32)


def dot_tn(a, b):
    return lax.dot_general(a, b, (((0,), (0,)), ((), ())), preferred_element_type=F32)


def kernel(
    frames, fsdp, heads_axis, width, features, lent,
    q_hbm, k_hbm, v_hbm, ck_hbm, cv_hbm, gq_hbm, gk_hbm, g_hbm,
    att_out, dq_out, dk_out, dv_out, gain_q_out, gain_k_out,
    tokens, gains, clean, flat_q, flat_k, inner_q, inner_k, rates,
    stats, sums1, sums2, far, far_rates, far_inner, far_sums, part, back_out, back_in,
    near_trip, far_trip, trip_out, trip_in, row_out, row_in,
    load_sem, own_send, relay_send, direct_recv, relay_recv, partner_recv, stats_send, stats_recv, sum_send, sum_recv,
    far_send, far_recv, back_send, grad_recv, att_recv, row_send, row_recv,
):
    q, k, v, g = [tokens.at[i] for i in range(4)]
    gq, gk = gains.at[0], gains.at[1]
    length = tokens.shape[1]
    head_count = width // DH
    kept = head_count - lent
    batch = lent // 2
    group = 2 - head_count % 2
    videos = fsdp // 2
    scaling = 1.0 / math.sqrt(DH)
    power = scaling * math.log2(math.e)
    frame = lax.axis_index("frame")
    fs = lax.axis_index("fsdp")
    half = fs // videos
    video = lax.rem(fs, videos)
    me1 = frame * videos + video
    n1 = frames * videos
    me2 = half * heads_axis + lax.axis_index("head")
    n2 = 2 * heads_axis

    def peer1(distance):
        p = lax.rem(me1 + distance, n1)
        return {"frame": p // videos, "fsdp": half * videos + lax.rem(p, videos)}

    def peer2(distance):
        p = lax.rem(me2 + distance, n2)
        return {"fsdp": (p // heads_axis) * videos + video, "head": lax.rem(p, heads_axis)}

    def columns(h):
        return pl.ds(pl.multiple_of(h * DH, DH), DH)

    def repeat(first, last, step):
        def body(i, _):
            step(i)
            return 0

        lax.fori_loop(first, last, body, 0)

    def arrive(ref, sem):
        pltpu.make_async_copy(ref, ref, sem).wait()

    for nb in range(frames - 1):

        @pl.when(frame == nb)
        def _():
            for kv, src in enumerate((ck_hbm, cv_hbm)):
                pltpu.make_async_copy(src, clean.at[nb, kv], load_sem.at[3]).start()

    barrier = pltpu.get_barrier_semaphore()

    def greet(d, _):
        pl.semaphore_signal(barrier, inc=1, device_id=peer1(d), device_id_type=MESH)
        return 0

    lax.fori_loop(1, n1, greet, 0)
    for d in range(1, n2):
        pl.semaphore_signal(barrier, inc=1, device_id=peer2(d), device_id_type=MESH)
    start = pl.multiple_of(me2 * width, DH)
    for src, dst, i in (
        (q_hbm, q, 0),
        (k_hbm, k, 0),
        (gq_hbm.at[:, pl.ds(start, width)], gq, 1),
        (gk_hbm.at[:, pl.ds(start, width)], gk, 1),
        (v_hbm, v, 2),
        (g_hbm, g, 2),
    ):
        pltpu.make_async_copy(src, dst, load_sem.at[i]).start()
    pl.semaphore_wait(barrier, n1 - 1 + n2 - 1)

    def frame_copy(src, dst, send, recv, target):
        return pltpu.make_async_remote_copy(
            src_ref=src,
            dst_ref=dst,
            send_sem=send,
            recv_sem=recv,
            device_id={"frame": jnp.int32(target)},
            device_id_type=MESH,
        )

    def direct_copy(j, h, target, send):
        land = clean.at[j, :, :, columns(h)]
        return frame_copy(land, land, send, direct_recv.at[j // 2, h], target)

    def relay_copy(j, h, target, send):
        land = clean.at[j, :, :, columns(h)]
        return frame_copy(land, land, send, relay_recv.at[j // 2, h], target)

    def partner_copy(j):
        land = clean.at[j] if j % 2 == 0 else clean.at[j, :, :, pl.ds(kept * DH, lent * DH)]
        return frame_copy(land, land, own_send.at[1], partner_recv.at[0], 2 * (j // 2) + 1 - j % 2)

    def kept_heads(j, sem):
        land = clean.at[j, :, :, pl.ds(0, kept * DH)]
        return frame_copy(land, land, sem, partner_recv.at[0], (j + 1) % frames)

    def plan(nb):
        pair, side = nb // 2, nb % 2
        partner, further = 2 * pair + 1 - side, nb + 2
        direct = [2 * c + side for c in range(pair)]
        relayed = [2 * c + 1 - side for c in range(pair)]
        return direct, relayed, partner, further if further < frames else None

    def helps(nb):
        return lent > 0 and nb < 2

    def helped(nb):
        return lent > 0 and nb >= 2

    def has_partner_copy(nb):
        return nb % 2 == 0 or helps(nb)

    def send_own(nb, first, last):
        further = plan(nb)[3]
        repeat(first, last, lambda h: direct_copy(nb, h, further, own_send.at[0]).start())

    def far_copy(kind, r, target):
        src = (q_hbm, g_hbm)[kind].at[:, columns(kept + r)]
        return frame_copy(src, far.at[r, kind], far_send.at[0], far_recv.at[r], target)

    def back_copy(kind, r, target):
        recv = grad_recv.at[0] if kind == 0 else att_recv.at[r]
        return frame_copy(back_out.at[kind, r], back_in.at[kind, r], back_send.at[0], recv, target)

    def trip_copy(p, target):
        return frame_copy(trip_out.at[p], trip_in.at[p], row_send.at[1 + p], row_recv.at[1 + p], target)

    def row_copy(target):
        return frame_copy(row_out, row_in, row_send.at[0], row_recv.at[0], target)

    def lend(nb, first, last):
        def go(r):
            for kind in range(2):
                far_copy(kind, r, nb - 2).start()

        repeat(first, last, go)

    for nb in range(frames):

        @pl.when(frame == nb)
        def _():
            if helped(nb):
                lend(nb, 0, batch)
            if nb < frames - 1:
                arrive(clean.at[nb], load_sem.at[3])
            if plan(nb)[3] is not None:
                send_own(nb, 0, kept - 2 if helps(nb) else kept)
            if has_partner_copy(nb):
                partner_copy(nb).start()

    row = lax.broadcasted_iota(jnp.int32, (8, length), 0)

    def as_rows(a, b):
        a = jnp.sum(jnp.transpose(a), axis=0, keepdims=True)
        b = jnp.sum(jnp.transpose(b), axis=0, keepdims=True)
        return jnp.where(row == 0, a, jnp.where(row == 1, b, 0.0))

    def stats_copy(phase, d, part):
        return pltpu.make_async_remote_copy(
            src_ref=part,
            dst_ref=part,
            send_sem=stats_send.at[phase],
            recv_sem=stats_recv.at[phase],
            device_id=peer2(d),
            device_id_type=MESH,
        )

    def all_stats(phase):
        return stats_copy(phase, 1, stats.at[phase, pl.ds(0, n2 - 1)])

    def stats_go(phase, value):
        stats[phase, me2] = value
        for d in range(1, n2):
            stats_copy(phase, d, stats.at[phase, me2]).start()

    def stats_total(phase):
        all_stats(phase).wait_recv()
        return jnp.sum(stats[phase], axis=0)

    arrive(tokens.at[pl.ds(0, 2)], load_sem.at[0])

    def square(ref):
        total = jnp.zeros((length, DH), F32)
        for h in range(head_count):
            x = ref[:, h * DH : (h + 1) * DH].astype(F32)
            total = total + x * x
        return total

    stats_go(0, as_rows(square(q), square(k)))
    inner_q[...] = jnp.zeros_like(inner_q)
    inner_k[...] = jnp.zeros_like(inner_k)
    arrive(gains, load_sem.at[1])
    arrive(tokens.at[pl.ds(2, 2)], load_sem.at[2])
    rate_rows = lax.rsqrt(stats_total(0) / features + EPSILON)
    rates[...] = jnp.transpose(rate_rows)
    for nb in range(frames):
        if helped(nb):

            @pl.when(frame == nb)
            def _():
                row_out[...] = rate_rows
                row_copy(nb - 2).start()
                lend(nb, batch, lent)

    def store_grads(cols, q_full, k_full, grad_qn, grad_kn):
        fq = grad_qn * gq[:, cols]
        fk = grad_kn * gk[:, cols]
        flat_q[:, cols] = fq
        flat_k[:, cols] = fk
        inner_q[...] += q_full * fq
        inner_k[...] += k_full * fk
        sums1[me1, 0:1, cols] = jnp.sum(grad_qn * q_full * rates[:, 0:1], axis=0, keepdims=True)
        sums1[me1, 1:2, cols] = jnp.sum(grad_kn * k_full * rates[:, 1:2], axis=0, keepdims=True)

    def pass_on(nb, h):
        direct, _, partner, further = plan(nb)
        for j in direct:
            direct_copy(j, h, partner, relay_send.at[0, j // 2]).wait_recv()
            relay_copy(j, h, partner, relay_send.at[0, j // 2]).start()
            if further is not None:
                direct_copy(j, h, further, relay_send.at[1, j // 2]).start()

    def row_sum(terms):
        return functools.reduce(jnp.add, [jnp.sum(t, axis=1, keepdims=True) for t in terms])

    def row_max(terms):
        return functools.reduce(jnp.maximum, [jnp.max(t, axis=1, keepdims=True) for t in terms])

    def weigh(blocks, operands):
        return functools.reduce(jnp.add, [dot_nn(b, o) for b, o in zip(blocks, operands)])

    def own_heads(nb, hs):
        _, relayed, partner, _ = plan(nb)
        cols = [columns(h) for h in hs]
        q_full = [q[:, c].astype(F32) for c in cols]
        k_full = [k[:, c].astype(F32) for c in cols]
        qn = [(x * rates[:, 0:1] * gq[:, c]).astype(BF16) for x, c in zip(q_full, cols)]
        kn = [(x * rates[:, 1:2] * gk[:, c]).astype(BF16) for x, c in zip(k_full, cols)]
        grad = [g[:, c] for c in cols]
        scores = [[dot_nt(a, b)] for a, b in zip(qn, kn)]
        grad_probs = [[dot_nt(a, v[:, c])] for a, c in zip(grad, cols)]
        for h in hs:
            for j in relayed:
                relay_copy(j, h, partner, relay_send.at[0, j // 2]).wait_recv()
        keys = [[b] + [clean[j, 0, :, c] for j in range(nb)] for b, c in zip(kn, cols)]
        values = [[v[:, c]] + [clean[j, 1, :, c] for j in range(nb)] for c in cols]
        for i in range(len(hs)):
            scores[i] += [dot_nt(qn[i], key) for key in keys[i][1:]]
            grad_probs[i] += [dot_nt(grad[i], val) for val in values[i][1:]]
        top = [row_max(s) for s in scores]
        expo = [[jnp.exp2((x - t) * power) for x in s] for s, t in zip(scores, top)]
        inverse = [1.0 / row_sum(e) for e in expo]
        summed = [weigh([x.astype(BF16) for x in e], val) for e, val in zip(expo, values)]
        attention = [s * i for s, i in zip(summed, inverse)]
        for c, a in zip(cols, attention):
            att_out[:, c] = a.astype(BF16)
        delta = [row_sum([x.astype(F32) * a]) for x, a in zip(grad, attention)]
        probs = [[x * i for x in e] for e, i in zip(expo, inverse)]
        grad_scores = [
            [(p * (d - x)).astype(BF16) for p, d in zip(ps, ds)] for ps, ds, x in zip(probs, grad_probs, delta)
        ]
        grad_qn = [weigh(s, key) * scaling for s, key in zip(grad_scores, keys)]
        store_blocks(cols, q_full, k_full, qn, grad, grad_qn, grad_scores, probs)

    def store_blocks(cols, q_full, k_full, qn, grad, grad_qn, grad_scores, probs):
        grad_kn = [dot_tn(s[0], a) * scaling for s, a in zip(grad_scores, qn)]
        grad_v = [dot_tn(p[0].astype(BF16), x) for p, x in zip(probs, grad)]
        for c, x in zip(cols, grad_v):
            dv_out[:, c] = x.astype(BF16)
        for args in zip(cols, q_full, k_full, grad_qn, grad_kn):
            store_grads(*args)

    def merged(mine, theirs):
        top1, total1, dot1 = [mine[:, i : i + 1] for i in range(3)]
        top2, total2, dot2 = [theirs[:, i : i + 1] for i in range(3)]
        top = jnp.maximum(top1, top2)
        weight1 = jnp.exp2((top1 - top) * power)
        weight2 = jnp.exp2((top2 - top) * power)
        inverse = 1.0 / (total1 * weight1 + total2 * weight2)
        delta = (dot1 * weight1 + dot2 * weight2) * inverse
        return top, inverse, delta, weight1 * inverse, total2 * weight2 * inverse

    def first_pass(rs, qn, grad, keys, values):
        scores = [[dot_nt(a, key) for key in ks] for a, ks in zip(qn, keys)]
        top = [row_max(s) for s in scores]
        expo = [[jnp.exp2((x - t) * power) for x in s] for s, t in zip(scores, top)]
        total = [row_sum(e) for e in expo]
        summed = [weigh([x.astype(BF16) for x in e], val) for e, val in zip(expo, values)]
        for i, r in enumerate(rs):
            near_trip[r, :, 0:1] = top[i]
            near_trip[r, :, 1:2] = total[i]
            near_trip[r, :, 2:3] = row_sum([grad[i].astype(F32) * summed[i]])
        return summed, total

    def second_pass(qn, grad, keys, values, merge):
        scores = [[dot_nt(a, key) for key in ks] for a, ks in zip(qn, keys)]
        grad_probs = [[dot_nt(a, val) for val in vs] for a, vs in zip(grad, values)]
        probs = [[jnp.exp2((x - m[0]) * power) * m[1] for x in s] for s, m in zip(scores, merge)]
        grad_scores = [
            [(p * (d - m[2])).astype(BF16) for p, d in zip(ps, ds)] for ps, ds, m in zip(probs, grad_probs, merge)
        ]
        return probs, grad_scores, [weigh(s, key) * scaling for s, key in zip(grad_scores, keys)]

    def trade(p, target):
        lane = lax.broadcasted_iota(jnp.int32, (length, DH), 1)
        packed = jnp.zeros((length, DH), F32)
        for r in range(batch):
            for i in range(3):
                packed = jnp.where(lane == 3 * r + i, near_trip[p * batch + r, :, i : i + 1], packed)
        trip_out[p] = jnp.transpose(packed)[: trip_out.shape[1]]
        trip_copy(p, target).start()

    def traded(p, target):
        trip_copy(p, target).wait_recv()
        unpacked = jnp.transpose(trip_in[p])
        for r in range(batch):
            for i in range(3):
                far_trip[p * batch + r, :, i : i + 1] = unpacked[:, 3 * r + i : 3 * r + i + 1]

    def batch_of(p):
        return [p * batch + r for r in range(batch)]

    def far_operands(r):
        cols = columns(kept + r)
        q_full = far[r, 0].astype(F32)
        rate, gain = far_rates[:, 0:1], gq[:, cols]
        keys = [clean[j, 0, :, cols] for j in range(2)]
        values = [clean[j, 1, :, cols] for j in range(2)]
        return cols, q_full, rate, gain, (q_full * rate * gain).astype(BF16), far[r, 1], keys, values

    def near_operands(nb, r):
        cols = columns(kept + r)
        q_full = q[:, cols].astype(F32)
        k_full = k[:, cols].astype(F32)
        qn = (q_full * rates[:, 0:1] * gq[:, cols]).astype(BF16)
        kn = (k_full * rates[:, 1:2] * gk[:, cols]).astype(BF16)
        keys = [kn] + [clean[j, 0, :, cols] for j in range(2, nb)]
        values = [v[:, cols]] + [clean[j, 1, :, cols] for j in range(2, nb)]
        return cols, q_full, k_full, qn, g[:, cols], keys, values

    def help_first(nb, rs):
        for r in rs:
            frame_copy(far.at[r], far.at[r], far_send.at[0], far_recv.at[r], nb + 2).wait_recv()
        _, _, _, _, qn, grad, keys, values = zip(*[far_operands(r) for r in rs])
        summed, total = first_pass(rs, qn, grad, keys, values)
        for i, r in enumerate(rs):
            back_out[1, r] = (summed[i] / total[i]).astype(BF16)

    def help_second(rs):
        cols, q_full, rate, gain, qn, grad, keys, values = zip(*[far_operands(r) for r in rs])
        merge = [merged(near_trip[r], far_trip[r]) for r in rs]
        _, _, grad_qn = second_pass(qn, grad, keys, values, merge)
        for i, r in enumerate(rs):
            back_out[0, r] = grad_qn[i].astype(BF16)
            far_inner[...] += q_full[i] * (grad_qn[i] * gain[i])
            far_sums[r : r + 1, :] = jnp.sum(grad_qn[i] * q_full[i] * rate[i], axis=0, keepdims=True)

    def near_first(nb, rs):
        _, _, _, qn, grad, keys, values = zip(*[near_operands(nb, r) for r in rs])
        summed, _ = first_pass(rs, qn, grad, keys, values)
        for i, r in enumerate(rs):
            part[r] = summed[i]

    def near_second(nb, rs):
        cols, q_full, k_full, qn, grad, keys, values = zip(*[near_operands(nb, r) for r in rs])
        merge = [merged(near_trip[r], far_trip[r]) for r in rs]
        probs, grad_scores, grad_qn = second_pass(qn, grad, keys, values, merge)
        store_blocks(cols, q_full, k_full, qn, grad, grad_qn, grad_scores, probs)
        for m, r in zip(merge, rs):
            part[r] = part[r] * m[3]
            far_trip[r, :, 3:4] = m[4]

    def s1_copy(d, part):
        return pltpu.make_async_remote_copy(
            src_ref=part,
            dst_ref=part,
            send_sem=sum_send.at[0],
            recv_sem=sum_recv.at[0],
            device_id=peer1(d),
            device_id_type=MESH,
        )

    def send_sums():
        repeat(1, n1, lambda d: s1_copy(d, sums1.at[me1]).start())

    def own_range(nb, first, last):
        repeat(first // group, last // group, lambda i: own_heads(nb, [group * i + x for x in range(group)]))

    for nb in range(frames):

        @pl.when(frame == nb)
        def _():
            if nb % 2 == 1:
                partner_copy(nb - 1).wait_recv()
            if helps(nb):
                other = nb + 2
                first = head_count * 2 // 5 // group * group
                middle = head_count * 3 // 5 // group * group
                own_range(nb, 0, first)
                if nb == 0:
                    partner_copy(1).wait_recv()
                row_copy(other).wait_recv()
                far_rates[...] = jnp.transpose(row_in[...])
                far_inner[...] = jnp.zeros_like(far_inner)
                help_first(nb, batch_of(0))
                trade(0, other)
                send_own(nb, kept - 2, kept)
                own_range(nb, first, middle)
                traded(0, other)
                help_second(batch_of(0))
                help_first(nb, batch_of(1))
                trade(1, other)
                repeat(0, batch, lambda r: back_copy(0, r, other).start())
                traded(1, other)
                help_second(batch_of(1))
                row_out[...] = as_rows(far_inner[...], jnp.zeros_like(far_inner))
                row_copy(other).start()
                repeat(batch, lent, lambda r: back_copy(0, r, other).start())
                own_range(nb, middle, head_count)
                for r in range(lent):
                    sums1[me1, 0:1, columns(kept + r)] += far_sums[r : r + 1, :]
                send_sums()
                repeat(0, lent, lambda r: back_copy(1, r, other).start())
                stats_go(1, as_rows(inner_q[...], inner_k[...]))
            elif helped(nb):
                other = nb - 2
                for p in range(2):
                    near_first(nb, batch_of(p))
                    trade(p, other)

                def step(h):
                    pass_on(nb, h)

                    @pl.when((h == kept // 2) | (h == kept - 1))
                    def _():
                        p = jnp.where(h == kept - 1, 1, 0)
                        traded(p, other)
                        near_second(nb, batch_of(p))

                    own_heads(nb, [h])

                repeat(0, kept, step)
                send_sums()
                row_copy(other).wait_recv()
                stats_go(1, as_rows(inner_q[...], inner_k[...]) + row_in[...])
            else:

                def step(h):
                    pass_on(nb, h)
                    own_heads(nb, [h])

                repeat(0, head_count, step)
                send_sums()
                stats_go(1, as_rows(inner_q[...], inner_k[...]))

    def s2_copy(d, part):
        return pltpu.make_async_remote_copy(
            src_ref=part,
            dst_ref=part,
            send_sem=sum_send.at[1],
            recv_sem=sum_recv.at[1],
            device_id=peer2(d),
            device_id_type=MESH,
        )

    all_s1 = s1_copy(1, sums1.at[pl.ds(0, n1 - 1)])
    all_s2 = s2_copy(1, sums2.at[pl.ds(0, n2 - 1)])
    inners = jnp.transpose(stats_total(1))
    rate_q = rates[:, 0:1]
    rate_k = rates[:, 1:2]
    cube_q = rate_q * rate_q * rate_q * inners[:, 0:1] / features
    cube_k = rate_k * rate_k * rate_k * inners[:, 1:2] / features

    all_s1.wait_recv()
    sums2[me2] = jnp.sum(sums1[...], axis=0)
    for d in range(1, n2):
        s2_copy(d, sums2.at[me2]).start()

    def finish(h, _):
        cols = columns(h)
        dq_out[:, cols] = (rate_q * flat_q[:, cols] - q[:, cols].astype(F32) * cube_q).astype(BF16)
        dk_out[:, cols] = (rate_k * flat_k[:, cols] - k[:, cols].astype(F32) * cube_k).astype(BF16)
        return 0

    lax.fori_loop(0, kept, finish, 0)
    for nb in range(frames):
        if helped(nb):

            @pl.when(frame == nb)
            def _():
                grads = back_in.at[0]
                frame_copy(grads, grads, back_send.at[0], grad_recv.at[0], nb - 2).wait_recv()

                def add(r):
                    cols = columns(kept + r)
                    flat_q[:, cols] += back_in[0, r].astype(F32) * gq[:, cols]

                repeat(0, lent, add)

    lax.fori_loop(kept, head_count, finish, 0)
    all_s2.wait_recv()
    for p in range(n2):
        gain_q_out[:, p * width : (p + 1) * width] = sums2[p, 0:1, :]
        gain_k_out[:, p * width : (p + 1) * width] = sums2[p, 1:2, :]

    for nb in range(frames):
        if helped(nb):

            @pl.when(frame == nb)
            def _():
                def join(r):
                    back_copy(1, r, nb - 2).wait_recv()
                    far = back_in[1, r].astype(F32) * far_trip[r, :, 3:4]
                    att_out[:, columns(kept + r)] = (part[r] + far).astype(BF16)

                repeat(0, lent, join)

    all_stats(0).wait_send()
    all_stats(1).wait_send()
    all_s1.wait_send()
    all_s2.wait_send()
    for nb in range(frames):
        direct, _, _, further = plan(nb)

        @pl.when(frame == nb)
        def _():
            if further is not None:
                kept_heads(nb, own_send.at[0]).wait_send()
            if has_partner_copy(nb):
                partner_copy(nb).wait_send()
            for j in direct:
                for t in range(1 if further is None else 2):
                    kept_heads(j, relay_send.at[t, j // 2]).wait_send()
            if helps(nb) or helped(nb):
                other = nb + 2 if helps(nb) else nb - 2
                for p in range(2):
                    trip_copy(p, other).wait_send()
                row_copy(other).wait_send()
            if helps(nb):
                frame_copy(back_out, back_in, back_send.at[0], grad_recv.at[0], nb + 2).wait_send()
            if helped(nb):
                frame_copy(far, far, far_send.at[0], far_recv.at[0], nb - 2).wait_send()


def write_out(*refs):
    sem = refs[12]
    copies = [pltpu.make_async_copy(refs[i], refs[6 + i], sem.at[i]) for i in range(6)]
    for copy in copies:
        copy.start()
    for copy in copies:
        copy.wait()


def on_device(queries, noisy_keys, noisy_values, clean_keys, clean_values, gain_query, gain_key, out_grad):
    length, width = queries.shape
    features = gain_query.shape[0]
    frames = lax.axis_size("frame")
    fsdp = lax.axis_size("fsdp")
    heads_axis = lax.axis_size("head")
    head_count = width // DH
    n1 = frames * (fsdp // 2)
    n2 = 2 * heads_axis
    block = pltpu.VMEM((length, width), BF16)
    gains = pltpu.VMEM((1, features), F32)
    anywhere = pl.BlockSpec(memory_space=pl.ANY)
    vmem = pl.BlockSpec(memory_space=pltpu.VMEM)
    dma = pltpu.SemaphoreType.DMA
    chips = max(frames // 2 - 1, 1)
    kept = 4 * 2 * length * width + 2 * 4 * features
    lent = head_count // 5 * 2 if frames == 4 else 0
    held = max(lent, 1)
    kept_count = head_count - lent
    trip_rows = -(-3 * (held // 2) // 8) * 8 if lent else 8
    outs = pl.pallas_call(
        functools.partial(kernel, frames, fsdp, heads_axis, width, features, lent),
        out_shape=(block, block, block, block, gains, gains),
        in_specs=[anywhere] * 8,
        out_specs=[vmem] * 6,
        scratch_shapes=[
            pltpu.VMEM((4, length, width), BF16),
            pltpu.VMEM((2, 1, width), F32),
            pltpu.VMEM((frames, 2, length, width), BF16),
            pltpu.VMEM((length, width), F32),
            pltpu.VMEM((length, width), F32),
            pltpu.VMEM((length, DH), F32),
            pltpu.VMEM((length, DH), F32),
            pltpu.VMEM((length, 8), F32),
            pltpu.VMEM((2, n2, 8, length), F32),
            pltpu.VMEM((n1, 2, width), F32),
            pltpu.VMEM((n2, 2, width), F32),
            pltpu.VMEM((held, 2, length, DH), BF16),
            pltpu.VMEM((length, 8), F32),
            pltpu.VMEM((length, DH), F32),
            pltpu.VMEM((-(-held // 8) * 8, DH), F32),
            pltpu.VMEM((held, length, DH), F32),
            pltpu.VMEM((2, held, length, DH), BF16),
            pltpu.VMEM((2, held, length, DH), BF16),
            pltpu.VMEM((held, length, 8), F32),
            pltpu.VMEM((held, length, 8), F32),
            pltpu.VMEM((2, trip_rows, length), F32),
            pltpu.VMEM((2, trip_rows, length), F32),
            pltpu.VMEM((8, length), F32),
            pltpu.VMEM((8, length), F32),
            dma((4,)),
            dma((2,)),
            dma((2, chips)),
            dma((chips, kept_count)),
            dma((chips, kept_count)),
            dma((1,)),
            dma((2,)),
            dma((2,)),
            dma((2,)),
            dma((2,)),
            dma((1,)),
            dma((held,)),
            dma((1,)),
            dma((1,)),
            dma((held,)),
            dma((3,)),
            dma((3,)),
        ],
        compiler_params=pltpu.CompilerParams(
            collective_id=0, has_side_effects=True, vmem_limit_bytes=VMEM_BYTES - kept - 4096
        ),
        name="attention",
    )(
        queries, noisy_keys, noisy_values, clean_keys, clean_values,
        gain_query.reshape(1, features), gain_key.reshape(1, features), out_grad,
    )
    outs = pl.pallas_call(
        write_out,
        out_shape=tuple(jax.ShapeDtypeStruct(out.shape, out.dtype) for out in outs),
        in_specs=[anywhere] * 6,
        out_specs=[anywhere] * 6,
        scratch_shapes=[dma((6,))],
        compiler_params=pltpu.CompilerParams(vmem_limit_bytes=8 * 1024 * 1024),
        name="write_out",
    )(*outs)
    return (*outs[:4], outs[4].reshape(features), outs[5].reshape(features))


def solution(mesh):
    tokens = P("frame", ("fsdp", "head"))
    return jax.shard_map(
        on_device,
        mesh=mesh,
        in_specs=(tokens, tokens, tokens, tokens, tokens, P(), P(), tokens),
        out_specs=(tokens, tokens, tokens, tokens, P(), P()),
        check_vma=False,
    )
```

```python
import functools
import math

import jax
import jax.numpy as jnp
from jax import lax
from jax.experimental import pallas as pl
from jax.experimental.pallas import tpu as pltpu
from jax.sharding import PartitionSpec as P

DH = 128
EPSILON = 1e-06
MESH = pl.DeviceIdType.MESH
VMEM_BYTES = 67043328
F32 = jnp.float32
BF16 = jnp.bfloat16


def dot_nt(a, b):
    return lax.dot_general(a, b, (((1,), (1,)), ((), ())), preferred_element_type=F32)


def dot_nn(a, b):
    return lax.dot_general(a, b, (((1,), (0,)), ((), ())), preferred_element_type=F32)


def dot_tn(a, b):
    return lax.dot_general(a, b, (((0,), (0,)), ((), ())), preferred_element_type=F32)


def kernel(
    frames, fsdp, heads_axis, width, features, lent,
    q_hbm, k_hbm, v_hbm, ck_hbm, cv_hbm, gq_hbm, gk_hbm, g_hbm,
    att_out, dq_out, dk_out, dv_out, gain_q_out, gain_k_out,
    tokens, gains, clean, flat_q, flat_k, inner_q, inner_k, rates,
    stats, sums, sums1, sums2, ends, far_sum, far, far_rates, far_inner, far_sums, part, back_out, back_in,
    near_trip, far_trip, trip_out, trip_in, row_out, row_in,
    load_sem, own_send, relay_send, direct_recv, relay_recv, partner_recv, stats_send, stats_recv, sum_send, sum_recv,
    far_send, far_recv, back_send, grad_recv, att_recv, row_send, row_recv, end_send, end_recv,
):
    q, k, v, g = [tokens.at[i] for i in range(4)]
    gq, gk = gains.at[0], gains.at[1]
    length = tokens.shape[1]
    head_count = width // DH
    devices = frames * fsdp * heads_axis
    kept = head_count - lent
    batch = lent // 2
    group = 2 - head_count % 2
    videos = fsdp // 2
    scaling = 1.0 / math.sqrt(DH)
    power = scaling * math.log2(math.e)
    frame = lax.axis_index("frame")
    fs = lax.axis_index("fsdp")
    half = fs // videos
    video = lax.rem(fs, videos)
    me1 = frame * videos + video
    n1 = frames * videos
    me2 = half * heads_axis + lax.axis_index("head")
    n2 = 2 * heads_axis

    def peer1(distance):
        p = lax.rem(me1 + distance, n1)
        return {"frame": p // videos, "fsdp": half * videos + lax.rem(p, videos)}

    def peer2(distance):
        p = lax.rem(me2 + distance, n2)
        return {"fsdp": (p // heads_axis) * videos + video, "head": lax.rem(p, heads_axis)}

    def columns(h):
        return pl.ds(pl.multiple_of(h * DH, DH), DH)

    def repeat(first, last, step):
        def body(i, _):
            step(i)
            return 0

        lax.fori_loop(first, last, body, 0)

    def arrive(ref, sem):
        pltpu.make_async_copy(ref, ref, sem).wait()

    for nb in range(frames - 1):

        @pl.when(frame == nb)
        def _():
            for kv, src in enumerate((ck_hbm, cv_hbm)):
                pltpu.make_async_copy(src, clean.at[nb, kv], load_sem.at[3]).start()

    barrier = pltpu.get_barrier_semaphore()

    def greet(d, _):
        pl.semaphore_signal(barrier, inc=1, device_id=peer1(d), device_id_type=MESH)
        return 0

    lax.fori_loop(1, n1, greet, 0)
    for d in range(1, n2):
        pl.semaphore_signal(barrier, inc=1, device_id=peer2(d), device_id_type=MESH)
    start = pl.multiple_of(me2 * width, DH)
    for src, dst, i in (
        (q_hbm, q, 0),
        (k_hbm, k, 0),
        (gq_hbm.at[:, pl.ds(start, width)], gq, 1),
        (gk_hbm.at[:, pl.ds(start, width)], gk, 1),
        (v_hbm, v, 2),
        (g_hbm, g, 2),
    ):
        pltpu.make_async_copy(src, dst, load_sem.at[i]).start()
    pl.semaphore_wait(barrier, n1 - 1 + n2 - 1)

    def frame_copy(src, dst, send, recv, target):
        return pltpu.make_async_remote_copy(
            src_ref=src,
            dst_ref=dst,
            send_sem=send,
            recv_sem=recv,
            device_id={"frame": jnp.int32(target)},
            device_id_type=MESH,
        )

    def direct_copy(j, h, target, send):
        land = clean.at[j, :, :, columns(h)]
        return frame_copy(land, land, send, direct_recv.at[j // 2, h], target)

    def relay_copy(j, h, target, send):
        land = clean.at[j, :, :, columns(h)]
        return frame_copy(land, land, send, relay_recv.at[j // 2, h], target)

    def partner_copy(j):
        land = clean.at[j] if j % 2 == 0 else clean.at[j, :, :, pl.ds(kept * DH, lent * DH)]
        return frame_copy(land, land, own_send.at[1], partner_recv.at[0], 2 * (j // 2) + 1 - j % 2)

    def kept_heads(j, sem):
        land = clean.at[j, :, :, pl.ds(0, kept * DH)]
        return frame_copy(land, land, sem, partner_recv.at[0], (j + 1) % frames)

    def plan(nb):
        pair, side = nb // 2, nb % 2
        partner, further = 2 * pair + 1 - side, nb + 2
        direct = [2 * c + side for c in range(pair)]
        relayed = [2 * c + 1 - side for c in range(pair)]
        return direct, relayed, partner, further if further < frames else None

    def helps(nb):
        return lent > 0 and nb < 2

    def helped(nb):
        return lent > 0 and nb >= 2

    def has_partner_copy(nb):
        return nb % 2 == 0 or helps(nb)

    def send_own(nb, first, last):
        further = plan(nb)[3]
        repeat(first, last, lambda h: direct_copy(nb, h, further, own_send.at[0]).start())

    def far_copy(kind, r, p, target):
        src = (q_hbm, g_hbm)[kind].at[:, columns(kept + r)]
        return frame_copy(src, far.at[r, kind], far_send.at[0], far_recv.at[p], target)

    def back_copy(kind, r, target):
        recv = grad_recv.at[0] if kind == 0 else att_recv.at[r]
        return frame_copy(back_out.at[kind, r], back_in.at[kind, r], back_send.at[0], recv, target)

    def trip_copy(p, target):
        return frame_copy(trip_out.at[p], trip_in.at[p], row_send.at[1], row_recv.at[1 + p], target)

    def sum_copy(target):
        return frame_copy(sums, far_sum, row_send.at[2], row_recv.at[3], target)

    def row_copy(target):
        return frame_copy(row_out, row_in, row_send.at[0], row_recv.at[0], target)

    def lend(nb, p):
        def go(r):
            for kind in range(2):
                far_copy(kind, r, p, nb - 2).start()

        repeat(p * batch, (p + 1) * batch, go)

    for nb in range(frames):

        @pl.when(frame == nb)
        def _():
            if helped(nb):
                lend(nb, 0)
            if nb < frames - 1:
                arrive(clean.at[nb], load_sem.at[3])
            if plan(nb)[3] is not None:
                send_own(nb, 0, kept - 2 if helps(nb) else kept)
            if has_partner_copy(nb):
                partner_copy(nb).start()

    row = lax.broadcasted_iota(jnp.int32, (8, length), 0)

    def as_rows(a, b):
        a = jnp.sum(jnp.transpose(a), axis=0, keepdims=True)
        b = jnp.sum(jnp.transpose(b), axis=0, keepdims=True)
        return jnp.where(row == 0, a, jnp.where(row == 1, b, 0.0))

    def stats_copy(phase, d, part):
        return pltpu.make_async_remote_copy(
            src_ref=part,
            dst_ref=part,
            send_sem=stats_send.at[0],
            recv_sem=stats_recv.at[phase],
            device_id=peer2(d),
            device_id_type=MESH,
        )

    def all_stats(phase):
        return stats_copy(phase, 1, stats.at[phase, pl.ds(0, n2 - 1)])

    def stats_go(phase, value):
        stats[phase, me2] = value
        for d in range(1, n2):
            stats_copy(phase, d, stats.at[phase, me2]).start()

    def stats_total(phase):
        all_stats(phase).wait_recv()
        return jnp.sum(stats[phase], axis=0)

    arrive(tokens.at[pl.ds(0, 2)], load_sem.at[0])

    def square(ref):
        total = jnp.zeros((length, DH), F32)
        for h in range(head_count):
            x = ref[:, h * DH : (h + 1) * DH].astype(F32)
            total = total + x * x
        return total

    stats_go(0, as_rows(square(q), square(k)))
    inner_q[...] = jnp.zeros_like(inner_q)
    inner_k[...] = jnp.zeros_like(inner_k)
    arrive(gains, load_sem.at[1])
    arrive(tokens.at[pl.ds(2, 2)], load_sem.at[2])
    rate_rows = lax.rsqrt(stats_total(0) / features + EPSILON)
    rates[...] = jnp.transpose(rate_rows)
    for nb in range(frames):
        if helped(nb):

            @pl.when(frame == nb)
            def _():
                row_out[...] = rate_rows[0:2]
                row_copy(nb - 2).start()
                lend(nb, 1)

    def store_grads(cols, q_full, k_full, grad_qn, grad_kn):
        fq = grad_qn * gq[:, cols]
        fk = grad_kn * gk[:, cols]
        flat_q[:, cols] = fq
        flat_k[:, cols] = fk
        inner_q[...] += q_full * fq
        inner_k[...] += k_full * fk
        sums[0:1, cols] = jnp.sum(grad_qn * q_full * rates[:, 0:1], axis=0, keepdims=True)
        sums[1:2, cols] = jnp.sum(grad_kn * k_full * rates[:, 1:2], axis=0, keepdims=True)

    def pass_on(nb, h):
        direct, _, partner, further = plan(nb)
        for j in direct:
            direct_copy(j, h, partner, relay_send.at[0, j // 2]).wait_recv()
            relay_copy(j, h, partner, relay_send.at[0, j // 2]).start()
            if further is not None:
                direct_copy(j, h, further, relay_send.at[1, j // 2]).start()

    def row_sum(terms):
        return functools.reduce(jnp.add, [jnp.sum(t, axis=1, keepdims=True) for t in terms])

    def row_max(terms):
        return functools.reduce(jnp.maximum, [jnp.max(t, axis=1, keepdims=True) for t in terms])

    def weigh(blocks, operands):
        return functools.reduce(jnp.add, [dot_nn(b, o) for b, o in zip(blocks, operands)])

    def own_heads(nb, hs):
        _, relayed, partner, _ = plan(nb)
        cols = [columns(h) for h in hs]
        q_full = [q[:, c].astype(F32) for c in cols]
        k_full = [k[:, c].astype(F32) for c in cols]
        qn = [(x * rates[:, 0:1] * gq[:, c]).astype(BF16) for x, c in zip(q_full, cols)]
        kn = [(x * rates[:, 1:2] * gk[:, c]).astype(BF16) for x, c in zip(k_full, cols)]
        grad = [g[:, c] for c in cols]
        scores = [[dot_nt(a, b)] for a, b in zip(qn, kn)]
        grad_probs = [[dot_nt(a, v[:, c])] for a, c in zip(grad, cols)]
        for h in hs:
            for j in relayed:
                relay_copy(j, h, partner, relay_send.at[0, j // 2]).wait_recv()
        keys = [[b] + [clean[j, 0, :, c] for j in range(nb)] for b, c in zip(kn, cols)]
        values = [[v[:, c]] + [clean[j, 1, :, c] for j in range(nb)] for c in cols]
        for i in range(len(hs)):
            scores[i] += [dot_nt(qn[i], key) for key in keys[i][1:]]
            grad_probs[i] += [dot_nt(grad[i], val) for val in values[i][1:]]
        top = [row_max(s) for s in scores]
        expo = [[jnp.exp2((x - t) * power) for x in s] for s, t in zip(scores, top)]
        inverse = [1.0 / row_sum(e) for e in expo]
        summed = [weigh([x.astype(BF16) for x in e], val) for e, val in zip(expo, values)]
        attention = [s * i for s, i in zip(summed, inverse)]
        for c, a in zip(cols, attention):
            att_out[:, c] = a.astype(BF16)
        delta = [row_sum([x.astype(F32) * a]) for x, a in zip(grad, attention)]
        probs = [[x * i for x in e] for e, i in zip(expo, inverse)]
        grad_scores = [
            [(p * (d - x)).astype(BF16) for p, d in zip(ps, ds)] for ps, ds, x in zip(probs, grad_probs, delta)
        ]
        grad_qn = [weigh(s, key) * scaling for s, key in zip(grad_scores, keys)]
        store_blocks(cols, q_full, k_full, qn, grad, grad_qn, grad_scores, probs)

    def store_blocks(cols, q_full, k_full, qn, grad, grad_qn, grad_scores, probs):
        grad_kn = [dot_tn(s[0], a) * scaling for s, a in zip(grad_scores, qn)]
        grad_v = [dot_tn(p[0].astype(BF16), x) for p, x in zip(probs, grad)]
        for c, x in zip(cols, grad_v):
            dv_out[:, c] = x.astype(BF16)
        for args in zip(cols, q_full, k_full, grad_qn, grad_kn):
            store_grads(*args)

    def merged(mine, theirs):
        top1, total1, dot1 = [mine[:, i : i + 1] for i in range(3)]
        top2, total2, dot2 = [theirs[:, i : i + 1] for i in range(3)]
        top = jnp.maximum(top1, top2)
        weight1 = jnp.exp2((top1 - top) * power)
        weight2 = jnp.exp2((top2 - top) * power)
        inverse = 1.0 / (total1 * weight1 + total2 * weight2)
        delta = (dot1 * weight1 + dot2 * weight2) * inverse
        return top, inverse, delta, weight1 * inverse, total2 * weight2 * inverse

    def first_pass(rs, qn, grad, keys, values):
        scores = [[dot_nt(a, key) for key in ks] for a, ks in zip(qn, keys)]
        top = [row_max(s) for s in scores]
        expo = [[jnp.exp2((x - t) * power) for x in s] for s, t in zip(scores, top)]
        total = [row_sum(e) for e in expo]
        summed = [weigh([x.astype(BF16) for x in e], val) for e, val in zip(expo, values)]
        for i, r in enumerate(rs):
            near_trip[r, :, 0:1] = top[i]
            near_trip[r, :, 1:2] = total[i]
            near_trip[r, :, 2:3] = row_sum([grad[i].astype(F32) * summed[i]])
        return summed, total

    def second_pass(qn, grad, keys, values, merge):
        scores = [[dot_nt(a, key) for key in ks] for a, ks in zip(qn, keys)]
        grad_probs = [[dot_nt(a, val) for val in vs] for a, vs in zip(grad, values)]
        probs = [[jnp.exp2((x - m[0]) * power) * m[1] for x in s] for s, m in zip(scores, merge)]
        grad_scores = [
            [(p * (d - m[2])).astype(BF16) for p, d in zip(ps, ds)] for ps, ds, m in zip(probs, grad_probs, merge)
        ]
        return probs, grad_scores, [weigh(s, key) * scaling for s, key in zip(grad_scores, keys)]

    def trade(p, target):
        lane = lax.broadcasted_iota(jnp.int32, (length, DH), 1)
        packed = jnp.zeros((length, DH), F32)
        for r in range(batch):
            for i in range(3):
                packed = jnp.where(lane == 3 * r + i, near_trip[p * batch + r, :, i : i + 1], packed)
        trip_out[p] = jnp.transpose(packed)[: trip_out.shape[1]]
        trip_copy(p, target).start()

    def traded(p, target):
        trip_copy(p, target).wait_recv()
        unpacked = jnp.transpose(trip_in[p])
        for r in range(batch):
            for i in range(3):
                far_trip[p * batch + r, :, i : i + 1] = unpacked[:, 3 * r + i : 3 * r + i + 1]

    def batch_of(p):
        return [p * batch + r for r in range(batch)]

    def far_operands(r):
        cols = columns(kept + r)
        q_full = far[r, 0].astype(F32)
        rate, gain = far_rates[:, 0:1], gq[:, cols]
        keys = [clean[j, 0, :, cols] for j in range(2)]
        values = [clean[j, 1, :, cols] for j in range(2)]
        return cols, q_full, rate, gain, (q_full * rate * gain).astype(BF16), far[r, 1], keys, values

    def near_operands(nb, r):
        cols = columns(kept + r)
        q_full = q[:, cols].astype(F32)
        k_full = k[:, cols].astype(F32)
        qn = (q_full * rates[:, 0:1] * gq[:, cols]).astype(BF16)
        kn = (k_full * rates[:, 1:2] * gk[:, cols]).astype(BF16)
        keys = [kn] + [clean[j, 0, :, cols] for j in range(2, nb)]
        values = [v[:, cols]] + [clean[j, 1, :, cols] for j in range(2, nb)]
        return cols, q_full, k_full, qn, g[:, cols], keys, values

    def help_first(nb, p):
        rs = batch_of(p)
        land = far.at[pl.ds(p * batch, batch)]
        frame_copy(land, land, far_send.at[0], far_recv.at[p], nb + 2).wait_recv()
        _, _, _, _, qn, grad, keys, values = zip(*[far_operands(r) for r in rs])
        summed, total = first_pass(rs, qn, grad, keys, values)
        for i, r in enumerate(rs):
            back_out[1, r] = (summed[i] / total[i]).astype(BF16)

    def help_second(rs):
        cols, q_full, rate, gain, qn, grad, keys, values = zip(*[far_operands(r) for r in rs])
        merge = [merged(near_trip[r], far_trip[r]) for r in rs]
        _, _, grad_qn = second_pass(qn, grad, keys, values, merge)
        for i, r in enumerate(rs):
            back_out[0, r] = grad_qn[i].astype(BF16)
            far_inner[...] += q_full[i] * (grad_qn[i] * gain[i])
            far_sums[r : r + 1, :] = jnp.sum(grad_qn[i] * q_full[i] * rate[i], axis=0, keepdims=True)

    def near_first(nb, rs):
        _, _, _, qn, grad, keys, values = zip(*[near_operands(nb, r) for r in rs])
        summed, _ = first_pass(rs, qn, grad, keys, values)
        for i, r in enumerate(rs):
            part[r] = summed[i]

    def near_second(nb, rs):
        cols, q_full, k_full, qn, grad, keys, values = zip(*[near_operands(nb, r) for r in rs])
        merge = [merged(near_trip[r], far_trip[r]) for r in rs]
        probs, grad_scores, grad_qn = second_pass(qn, grad, keys, values, merge)
        store_blocks(cols, q_full, k_full, qn, grad, grad_qn, grad_scores, probs)
        for m, r in zip(merge, rs):
            part[r] = part[r] * m[3]
            far_trip[r, :, 3:4] = m[4]

    def s1_copy(d, part):
        return pltpu.make_async_remote_copy(
            src_ref=part,
            dst_ref=part,
            send_sem=sum_send.at[0],
            recv_sem=sum_recv.at[0],
            device_id=peer1(d),
            device_id_type=MESH,
        )

    slots = 2 * videos if lent else n1
    high = me1 - n1 + slots

    def send_sums(addend):
        sums1[high] = sums[...] + addend
        repeat(1, n1, lambda d: s1_copy(d, sums1.at[high]).start())

    def end_copy(d, part):
        p = lax.rem((frame * fsdp + fs) * heads_axis + lax.axis_index("head") + d, devices)
        return pltpu.make_async_remote_copy(
            src_ref=part,
            dst_ref=part,
            send_sem=end_send.at[0],
            recv_sem=end_recv.at[0],
            device_id={
                "frame": p // (fsdp * heads_axis),
                "fsdp": lax.rem(p // heads_axis, fsdp),
                "head": lax.rem(p, heads_axis),
            },
            device_id_type=MESH,
        )

    last = pl.ds((kept - 1) * DH, DH)

    def own_range(nb, first, last):
        repeat(first // group, last // group, lambda i: own_heads(nb, [group * i + x for x in range(group)]))

    for nb in range(frames):

        @pl.when(frame == nb)
        def _():
            if nb % 2 == 1:
                partner_copy(nb - 1).wait_recv()
            if helps(nb):
                other = nb + 2
                first = head_count * 2 // 5 // group * group
                own_range(nb, 0, first)
                if nb == 0:
                    partner_copy(1).wait_recv()
                row_copy(other).wait_recv()
                far_rates[:, 0:2] = jnp.transpose(row_in[...])
                far_inner[...] = jnp.zeros_like(far_inner)
                help_first(nb, 0)
                trade(0, other)
                send_own(nb, kept - 2, kept)
                own_range(nb, first, head_count)
                traded(0, other)
                help_second(batch_of(0))
                help_first(nb, 1)
                trade(1, other)
                back_copy(0, 0, other).start()
                traded(1, other)
                help_second(batch_of(1))
                for r in range(lent):
                    sums[0:1, columns(kept + r)] += far_sums[r : r + 1, :]
                sum_copy(other).start()
                row_out[...] = as_rows(far_inner[...], jnp.zeros_like(far_inner))[0:2]
                row_copy(other).start()
                repeat(1, lent, lambda r: back_copy(0, r, other).start())
                repeat(0, lent, lambda r: back_copy(1, r, other).start())
                stats_go(1, as_rows(inner_q[...], inner_k[...]))
            elif helped(nb):
                other = nb - 2
                for p in range(2):
                    near_first(nb, batch_of(p))
                    trade(p, other)

                sums[:, last] = jnp.zeros((2, DH), F32)

                def step(h):
                    pass_on(nb, h)

                    @pl.when((h == kept // 2) | (h == kept - 1))
                    def _():
                        p = jnp.where(h == kept - 1, 1, 0)
                        traded(p, other)
                        near_second(nb, batch_of(p))

                    @pl.when(h == kept - 1)
                    def _():
                        sum_copy(other).wait_recv()
                        send_sums(far_sum[...])

                    own_heads(nb, [h])

                repeat(0, kept, step)
                row_copy(other).wait_recv()
                rows = as_rows(inner_q[...], inner_k[...])
                stats_go(1, jnp.where(row == 0, rows + row_in[0:1], rows))
                end = me2 * slots + high
                ends[end] = sums[:, last]
                repeat(1, devices, lambda d: end_copy(d, ends.at[end]).start())
            else:

                def step(h):
                    pass_on(nb, h)
                    own_heads(nb, [h])

                repeat(0, head_count, step)
                send_sums(0.0)
                stats_go(1, as_rows(inner_q[...], inner_k[...]))

    def s2_copy(d, part):
        return pltpu.make_async_remote_copy(
            src_ref=part,
            dst_ref=part,
            send_sem=sum_send.at[1],
            recv_sem=sum_recv.at[1],
            device_id=peer2(d),
            device_id_type=MESH,
        )

    def only(which, action):
        for nb in range(frames):
            if which(nb):
                pl.when(frame == nb)(action)

    all_s2 = s2_copy(1, sums2.at[pl.ds(0, n2 - 1)])
    if lent:
        only(helps, s1_copy(1, sums1.at[pl.ds(0, slots)]).wait_recv)
        only(helped, s1_copy(1, sums1.at[pl.ds(0, slots - 1)]).wait_recv)
    else:
        s1_copy(1, sums1.at[pl.ds(0, slots - 1)]).wait_recv()
    sums2[me2] = jnp.sum(sums1[pl.ds(0, slots)], axis=0)
    for d in range(1, n2):
        s2_copy(d, sums2.at[me2]).start()
    inners = jnp.transpose(stats_total(1))
    rate_q = rates[:, 0:1]
    rate_k = rates[:, 1:2]
    cube_q = rate_q * rate_q * rate_q * inners[:, 0:1] / features
    cube_k = rate_k * rate_k * rate_k * inners[:, 1:2] / features

    def finish(h, _):
        cols = columns(h)
        dq_out[:, cols] = (rate_q * flat_q[:, cols] - q[:, cols].astype(F32) * cube_q).astype(BF16)
        dk_out[:, cols] = (rate_k * flat_k[:, cols] - k[:, cols].astype(F32) * cube_k).astype(BF16)
        return 0

    lax.fori_loop(0, kept, finish, 0)
    for nb in range(frames):
        if helped(nb):

            @pl.when(frame == nb)
            def _():
                grads = back_in.at[0]
                frame_copy(grads, grads, back_send.at[0], grad_recv.at[0], nb - 2).wait_recv()

                def add(r):
                    cols = columns(kept + r)
                    flat_q[:, cols] += back_in[0, r].astype(F32) * gq[:, cols]

                repeat(0, lent, add)

    lax.fori_loop(kept, head_count, finish, 0)
    all_s2.wait_recv()
    for p in range(n2):
        gain_q_out[:, p * width : (p + 1) * width] = sums2[p, 0:1, :]
        gain_k_out[:, p * width : (p + 1) * width] = sums2[p, 1:2, :]
    if lent:
        only(helps, end_copy(1, ends.at[pl.ds(0, n2 * slots)]).wait_recv)
        only(helped, end_copy(1, ends.at[pl.ds(0, n2 * slots - 1)]).wait_recv)
        for p in range(n2):
            late = jnp.sum(ends[pl.ds(p * slots, slots)], axis=0)
            cols = pl.ds(p * width + (kept - 1) * DH, DH)
            gain_q_out[:, cols] += late[0:1]
            gain_k_out[:, cols] += late[1:2]

    for nb in range(frames):
        if helped(nb):

            @pl.when(frame == nb)
            def _():
                def join(r):
                    back_copy(1, r, nb - 2).wait_recv()
                    far = back_in[1, r].astype(F32) * far_trip[r, :, 3:4]
                    att_out[:, columns(kept + r)] = (part[r] + far).astype(BF16)

                repeat(0, lent, join)

    stats_copy(0, 1, stats.at[:, pl.ds(0, n2 - 1)]).wait_send()
    if lent:
        only(helped, s1_copy(1, sums1.at[pl.ds(0, n1 - 1)]).wait_send)
        only(helped, end_copy(1, ends.at[pl.ds(0, devices - 1)]).wait_send)
        only(helps, lambda: sum_copy(2).wait_send())
    else:
        s1_copy(1, sums1.at[pl.ds(0, n1 - 1)]).wait_send()
    all_s2.wait_send()
    for nb in range(frames):
        direct, _, _, further = plan(nb)

        @pl.when(frame == nb)
        def _():
            if further is not None:
                kept_heads(nb, own_send.at[0]).wait_send()
            if has_partner_copy(nb):
                partner_copy(nb).wait_send()
            for j in direct:
                for t in range(1 if further is None else 2):
                    kept_heads(j, relay_send.at[t, j // 2]).wait_send()
            if helps(nb) or helped(nb):
                other = nb + 2 if helps(nb) else nb - 2
                frame_copy(trip_out, trip_in, row_send.at[1], row_recv.at[1], other).wait_send()
                row_copy(other).wait_send()
            if helps(nb):
                frame_copy(back_out, back_in, back_send.at[0], grad_recv.at[0], nb + 2).wait_send()
            if helped(nb):
                frame_copy(far, far, far_send.at[0], far_recv.at[0], nb - 2).wait_send()


def write_out(*refs):
    sem = refs[12]
    copies = [pltpu.make_async_copy(refs[i], refs[6 + i], sem.at[i]) for i in range(6)]
    for copy in copies:
        copy.start()
    for copy in copies:
        copy.wait()


def on_device(queries, noisy_keys, noisy_values, clean_keys, clean_values, gain_query, gain_key, out_grad):
    length, width = queries.shape
    features = gain_query.shape[0]
    frames = lax.axis_size("frame")
    fsdp = lax.axis_size("fsdp")
    heads_axis = lax.axis_size("head")
    head_count = width // DH
    n1 = frames * (fsdp // 2)
    n2 = 2 * heads_axis
    block = pltpu.VMEM((length, width), BF16)
    gains = pltpu.VMEM((1, features), F32)
    anywhere = pl.BlockSpec(memory_space=pl.ANY)
    vmem = pl.BlockSpec(memory_space=pltpu.VMEM)
    dma = pltpu.SemaphoreType.DMA
    chips = max(frames // 2 - 1, 1)
    kept = 4 * 2 * length * width + 2 * 4 * features
    lent = head_count // 5 * 2 if frames == 4 else 0
    held = max(lent, 1)
    kept_count = head_count - lent
    trip_rows = -(-3 * (held // 2) // 8) * 8 if lent else 8
    outs = pl.pallas_call(
        functools.partial(kernel, frames, fsdp, heads_axis, width, features, lent),
        out_shape=(block, block, block, block, gains, gains),
        in_specs=[anywhere] * 8,
        out_specs=[vmem] * 6,
        scratch_shapes=[
            pltpu.VMEM((4, length, width), BF16),
            pltpu.VMEM((2, 1, width), F32),
            pltpu.VMEM((frames, 2, length, width), BF16),
            pltpu.VMEM((length, width), F32),
            pltpu.VMEM((length, width), F32),
            pltpu.VMEM((length, DH), F32),
            pltpu.VMEM((length, DH), F32),
            pltpu.VMEM((length, 8), F32),
            pltpu.VMEM((2, n2, 8, length), F32),
            pltpu.VMEM((2, width), F32),
            pltpu.VMEM((n1, 2, width), F32),
            pltpu.VMEM((n2, 2, width), F32),
            pltpu.VMEM((frames * fsdp * heads_axis if lent else 1, 2, DH), F32),
            pltpu.VMEM((2, width), F32),
            pltpu.VMEM((held, 2, length, DH), BF16),
            pltpu.VMEM((length, 8), F32),
            pltpu.VMEM((length, DH), F32),
            pltpu.VMEM((-(-held // 8) * 8, DH), F32),
            pltpu.VMEM((held, length, DH), F32),
            pltpu.VMEM((2, held, length, DH), BF16),
            pltpu.VMEM((2, held, length, DH), BF16),
            pltpu.VMEM((held, length, 8), F32),
            pltpu.VMEM((held, length, 8), F32),
            pltpu.VMEM((2, trip_rows, length), F32),
            pltpu.VMEM((2, trip_rows, length), F32),
            pltpu.VMEM((2, length), F32),
            pltpu.VMEM((2, length), F32),
            dma((4,)),
            dma((2,)),
            dma((min(chips, 2), chips)),
            dma((chips, kept_count)),
            dma((chips, kept_count)),
            dma((1,)),
            dma((1,)),
            dma((2,)),
            dma((2,)),
            dma((2,)),
            dma((1,)),
            dma((2,)),
            dma((1,)),
            dma((1,)),
            dma((held,)),
            dma((3,)),
            dma((4,)),
            dma((1,)),
            dma((1,)),
        ],
        compiler_params=pltpu.CompilerParams(
            collective_id=0, has_side_effects=True, vmem_limit_bytes=VMEM_BYTES - kept - 4096
        ),
        name="attention",
    )(
        queries, noisy_keys, noisy_values, clean_keys, clean_values,
        gain_query.reshape(1, features), gain_key.reshape(1, features), out_grad,
    )
    outs = pl.pallas_call(
        write_out,
        out_shape=tuple(jax.ShapeDtypeStruct(out.shape, out.dtype) for out in outs),
        in_specs=[anywhere] * 6,
        out_specs=[anywhere] * 6,
        scratch_shapes=[dma((6,))],
        compiler_params=pltpu.CompilerParams(vmem_limit_bytes=8 * 1024 * 1024),
        name="write_out",
    )(*outs)
    return (*outs[:4], outs[4].reshape(features), outs[5].reshape(features))


def solution(mesh):
    tokens = P("frame", ("fsdp", "head"))
    return jax.shard_map(
        on_device,
        mesh=mesh,
        in_specs=(tokens, tokens, tokens, tokens, tokens, P(), P(), tokens),
        out_specs=(tokens, tokens, tokens, tokens, P(), P()),
        check_vma=False,
    )
```

```python
import functools
import math

import jax
import jax.numpy as jnp
from jax import lax
from jax.experimental import pallas as pl
from jax.experimental.pallas import tpu as pltpu
from jax.sharding import PartitionSpec as P

DH = 128
EPSILON = 1e-06
MESH = pl.DeviceIdType.MESH
VMEM_BYTES = 67043328
F32 = jnp.float32
BF16 = jnp.bfloat16


def dot_nt(a, b):
    return lax.dot_general(a, b, (((1,), (1,)), ((), ())), preferred_element_type=F32)


def dot_nn(a, b):
    return lax.dot_general(a, b, (((1,), (0,)), ((), ())), preferred_element_type=F32)


def dot_tn(a, b):
    return lax.dot_general(a, b, (((0,), (0,)), ((), ())), preferred_element_type=F32)


def kernel(
    frames, fsdp, heads_axis, width, features, lent,
    q_hbm, k_hbm, v_hbm, ck_hbm, cv_hbm, gq_hbm, gk_hbm, g_hbm,
    att_out, dq_out, dk_out, dv_out, gain_q_out, gain_k_out,
    tokens, gains, clean, flat_q, flat_k, inner_q, inner_k, wide,
    stats, sums, sums1, sums2, ends, far_sum, far, far_wide, far_inner, far_sums, part, back_out, back_in,
    near_trip, far_trip, trip_out, trip_in, row_out, row_in,
    load_sem, own_send, relay_send, direct_recv, relay_recv, partner_recv, stats_send, stats_recv, sum_send, sum_recv,
    far_send, far_recv, back_send, grad_recv, att_recv, row_send, row_recv, end_send, end_recv, ready,
):
    q, k, v, g = [tokens.at[i] for i in range(4)]
    gq, gk = gains.at[0], gains.at[1]
    length = tokens.shape[1]
    head_count = width // DH
    devices = frames * fsdp * heads_axis
    kept = head_count - lent
    batches = [list(range(1, lent)), [0]]
    order = batches[0] + batches[1]
    group = 2 - head_count % 2
    videos = fsdp // 2
    scaling = 1.0 / math.sqrt(DH)
    power = scaling * math.log2(math.e)
    frame = lax.axis_index("frame")
    fs = lax.axis_index("fsdp")
    half = fs // videos
    video = lax.rem(fs, videos)
    me1 = frame * videos + video
    n1 = frames * videos
    me2 = half * heads_axis + lax.axis_index("head")
    n2 = 2 * heads_axis

    def peer1(distance):
        p = lax.rem(me1 + distance, n1)
        return {"frame": p // videos, "fsdp": half * videos + lax.rem(p, videos)}

    def peer2(distance):
        p = lax.rem(me2 + distance, n2)
        return {"fsdp": (p // heads_axis) * videos + video, "head": lax.rem(p, heads_axis)}

    def columns(h):
        return pl.ds(pl.multiple_of(h * DH, DH), DH)

    def repeat(first, last, step):
        def body(i, _):
            step(i)
            return 0

        lax.fori_loop(first, last, body, 0)

    def arrive(ref, sem):
        pltpu.make_async_copy(ref, ref, sem).wait()

    for nb in range(frames - 1):

        @pl.when(frame == nb)
        def _():
            for kv, src in enumerate((ck_hbm, cv_hbm)):
                pltpu.make_async_copy(src, clean.at[nb, kv], load_sem.at[3]).start()

    barrier = pltpu.get_barrier_semaphore()

    groups = videos - 1 + n2 - 1
    if lent:
        mates = [{"frame": jnp.int32(f)} for f in range(frames)]
        for f in range(frames):

            @pl.when(frame != f)
            def _():
                pl.semaphore_signal(barrier, inc=1, device_id=mates[f], device_id_type=MESH)

        for f in range(1, frames, 2):
            for d in range(1, videos):
                near = {"fsdp": half * videos + lax.rem(video + d, videos)}
                pl.semaphore_signal(barrier, inc=1, device_id={**near, **mates[f]}, device_id_type=MESH)
            for d in range(1, n2):
                pl.semaphore_signal(barrier, inc=1, device_id={**peer2(d), **mates[f]}, device_id_type=MESH)
    else:
        repeat(1, n1, lambda d: pl.semaphore_signal(barrier, inc=1, device_id=peer1(d), device_id_type=MESH))
        for d in range(1, n2):
            pl.semaphore_signal(barrier, inc=1, device_id=peer2(d), device_id_type=MESH)
    start = pl.multiple_of(me2 * width, DH)
    for src, dst, i in (
        (q_hbm, q, 0),
        (k_hbm, k, 0),
        (gq_hbm.at[:, pl.ds(start, width)], gq, 1),
        (gk_hbm.at[:, pl.ds(start, width)], gk, 1),
        (v_hbm, v, 2),
        (g_hbm, g, 2),
    ):
        pltpu.make_async_copy(src, dst, load_sem.at[i]).start()
    if lent:
        pl.semaphore_wait(barrier, frames - 1 + lax.rem(frame, 2) * (frames * groups))

        @pl.when(lax.rem(frame, 2) == 1)
        def _():
            pl.semaphore_signal(ready, inc=1, device_id={"frame": frame - 1}, device_id_type=MESH)

    else:
        pl.semaphore_wait(barrier, n1 - 1 + n2 - 1)

    def frame_copy(src, dst, send, recv, target):
        return pltpu.make_async_remote_copy(
            src_ref=src,
            dst_ref=dst,
            send_sem=send,
            recv_sem=recv,
            device_id={"frame": jnp.int32(target)},
            device_id_type=MESH,
        )

    def direct_copy(j, h, target, send):
        land = clean.at[j, :, :, columns(h)]
        return frame_copy(land, land, send, direct_recv.at[j // 2, h], target)

    def relay_copy(j, h, target, send):
        land = clean.at[j, :, :, columns(h)]
        return frame_copy(land, land, send, relay_recv.at[j // 2, h], target)

    def partner_copy(j):
        land = clean.at[j] if j % 2 == 0 else clean.at[j, :, :, pl.ds(kept * DH, lent * DH)]
        return frame_copy(land, land, own_send.at[1], partner_recv.at[0], 2 * (j // 2) + 1 - j % 2)

    def kept_heads(j, sem):
        land = clean.at[j, :, :, pl.ds(0, kept * DH)]
        return frame_copy(land, land, sem, partner_recv.at[0], (j + 1) % frames)

    def plan(nb):
        pair, side = nb // 2, nb % 2
        partner, further = 2 * pair + 1 - side, nb + 2
        direct = [2 * c + side for c in range(pair)]
        relayed = [2 * c + 1 - side for c in range(pair)]
        return direct, relayed, partner, further if further < frames else None

    def helps(nb):
        return lent > 0 and nb < 2

    def helped(nb):
        return lent > 0 and nb >= 2

    def has_partner_copy(nb):
        return nb % 2 == 0 or helps(nb)

    def send_own(nb, first, last):
        further = plan(nb)[3]
        repeat(first, last, lambda h: direct_copy(nb, h, further, own_send.at[0]).start())

    def far_copy(kind, r, target):
        src = (q_hbm, g_hbm)[kind].at[:, columns(kept + r)]
        return frame_copy(src, far.at[r, kind], far_send.at[0], far_recv.at[0 if r in batches[0] else 1], target)

    def back_copy(kind, r, target):
        recv = grad_recv.at[0] if kind == 0 else att_recv.at[r]
        return frame_copy(back_out.at[kind, r], back_in.at[kind, r], back_send.at[0], recv, target)

    def trip_copy(p, target):
        rs = pl.ds(batches[p][0], len(batches[p]))
        return frame_copy(trip_out.at[rs], trip_in.at[rs], row_send.at[1], row_recv.at[1 + p], target)

    def sum_copy(target):
        return frame_copy(sums, far_sum, row_send.at[2], row_recv.at[3], target)

    def row_copy(target):
        return frame_copy(row_out, row_in, row_send.at[0], row_recv.at[0], target)

    def lend(nb, first, last):
        for r in order[first:last]:
            for kind in range(2):
                far_copy(kind, r, nb - 2).start()

    for nb in range(frames):

        @pl.when(frame == nb)
        def _():
            if helped(nb):
                lend(nb, 0, lent // 2)
            if nb < frames - 1:
                arrive(clean.at[nb], load_sem.at[3])
            if plan(nb)[3] is not None:
                send_own(nb, 0, kept - 1 if helps(nb) else kept)
            if has_partner_copy(nb):
                partner_copy(nb).start()

    row = lax.broadcasted_iota(jnp.int32, (8, length), 0)

    def as_rows(a, b):
        a = jnp.sum(jnp.transpose(a), axis=0, keepdims=True)
        b = jnp.sum(jnp.transpose(b), axis=0, keepdims=True)
        return jnp.where(row == 0, a, jnp.where(row == 1, b, 0.0))

    def stats_copy(phase, d, part):
        return pltpu.make_async_remote_copy(
            src_ref=part,
            dst_ref=part,
            send_sem=stats_send.at[0],
            recv_sem=stats_recv.at[phase],
            device_id=peer2(d),
            device_id_type=MESH,
        )

    def all_stats(phase):
        return stats_copy(phase, 1, stats.at[phase, pl.ds(0, n2 - 1)])

    def stats_go(phase, value):
        stats[phase, me2] = value
        for d in range(1, n2):
            stats_copy(phase, d, stats.at[phase, me2]).start()

    def stats_total(phase):
        all_stats(phase).wait_recv()
        return jnp.sum(stats[phase], axis=0)

    arrive(tokens.at[pl.ds(0, 2)], load_sem.at[0])

    def square(ref):
        total = jnp.zeros((length, DH), F32)
        for h in range(head_count):
            x = ref[:, h * DH : (h + 1) * DH].astype(F32)
            total = total + x * x
        return total

    if lent:

        @pl.when(lax.rem(frame, 2) == 0)
        def _():
            pl.semaphore_wait(ready, 1)

    stats_go(0, as_rows(square(q), square(k)))
    inner_q[...] = jnp.zeros_like(inner_q)
    inner_k[...] = jnp.zeros_like(inner_k)
    arrive(gains, load_sem.at[1])
    arrive(tokens.at[pl.ds(2, 2)], load_sem.at[2])
    rate_rows = lax.rsqrt(stats_total(0) / features + EPSILON)
    rate_columns = jnp.transpose(rate_rows)
    for i in range(2):
        wide[i] = jnp.broadcast_to(rate_columns[:, i : i + 1], (length, DH))
    for nb in range(frames):
        if helped(nb):

            @pl.when(frame == nb)
            def _():
                row_out[...] = rate_rows[0:2]
                row_copy(nb - 2).start()
                lend(nb, lent // 2, lent)

    def store_grads(cols, q_full, k_full, grad_qn, grad_kn):
        fq = grad_qn * gq[:, cols]
        fk = grad_kn * gk[:, cols]
        flat_q[:, cols] = fq
        flat_k[:, cols] = fk
        inner_q[...] += q_full * fq
        inner_k[...] += k_full * fk
        sums[0:1, cols] = jnp.sum(grad_qn * q_full * wide[0], axis=0, keepdims=True)
        sums[1:2, cols] = jnp.sum(grad_kn * k_full * wide[1], axis=0, keepdims=True)

    def pass_on(nb, h):
        direct, _, partner, further = plan(nb)
        for j in direct:
            direct_copy(j, h, partner, relay_send.at[0, j // 2]).wait_recv()
            relay_copy(j, h, partner, relay_send.at[0, j // 2]).start()
            if further is not None:
                direct_copy(j, h, further, relay_send.at[1, j // 2]).start()

    def row_sum(terms):
        return functools.reduce(jnp.add, [jnp.sum(t, axis=1, keepdims=True) for t in terms])

    def row_max(terms):
        return functools.reduce(jnp.maximum, [jnp.max(t, axis=1, keepdims=True) for t in terms])

    def weigh(blocks, operands):
        return functools.reduce(jnp.add, [dot_nn(b, o) for b, o in zip(blocks, operands)])

    def own_heads(nb, hs):
        _, relayed, partner, _ = plan(nb)
        cols = [columns(h) for h in hs]
        q_full = [q[:, c].astype(F32) for c in cols]
        k_full = [k[:, c].astype(F32) for c in cols]
        qn = [(x * wide[0] * gq[:, c]).astype(BF16) for x, c in zip(q_full, cols)]
        kn = [(x * wide[1] * gk[:, c]).astype(BF16) for x, c in zip(k_full, cols)]
        grad = [g[:, c] for c in cols]
        scores = [[dot_nt(a, b)] for a, b in zip(qn, kn)]
        grad_probs = [[dot_nt(a, v[:, c])] for a, c in zip(grad, cols)]
        for h in hs:
            for j in relayed:
                relay_copy(j, h, partner, relay_send.at[0, j // 2]).wait_recv()
        keys = [[b] + [clean[j, 0, :, c] for j in range(nb)] for b, c in zip(kn, cols)]
        values = [[v[:, c]] + [clean[j, 1, :, c] for j in range(nb)] for c in cols]
        for i in range(len(hs)):
            scores[i] += [dot_nt(qn[i], key) for key in keys[i][1:]]
            grad_probs[i] += [dot_nt(grad[i], val) for val in values[i][1:]]
        top = [row_max(s) for s in scores]
        expo = [[jnp.exp2((x - t) * power) for x in s] for s, t in zip(scores, top)]
        inverse = [1.0 / row_sum(e) for e in expo]
        summed = [weigh([x.astype(BF16) for x in e], val) for e, val in zip(expo, values)]
        attention = [s * i for s, i in zip(summed, inverse)]
        for c, a in zip(cols, attention):
            att_out[:, c] = a.astype(BF16)
        delta = [row_sum([x.astype(F32) * a]) for x, a in zip(grad, attention)]
        probs = [[x * i for x in e] for e, i in zip(expo, inverse)]
        grad_scores = [
            [(p * (d - x)).astype(BF16) for p, d in zip(ps, ds)] for ps, ds, x in zip(probs, grad_probs, delta)
        ]
        grad_qn = [weigh(s, key) * scaling for s, key in zip(grad_scores, keys)]
        store_blocks(cols, q_full, k_full, qn, grad, grad_qn, grad_scores, probs)

    def store_blocks(cols, q_full, k_full, qn, grad, grad_qn, grad_scores, probs):
        grad_kn = [dot_tn(s[0], a) * scaling for s, a in zip(grad_scores, qn)]
        grad_v = [dot_tn(p[0].astype(BF16), x) for p, x in zip(probs, grad)]
        for c, x in zip(cols, grad_v):
            dv_out[:, c] = x.astype(BF16)
        for args in zip(cols, q_full, k_full, grad_qn, grad_kn):
            store_grads(*args)

    def merged(mine, theirs):
        top1, total1, dot1 = [mine[:, i : i + 1] for i in range(3)]
        top2, total2, dot2 = [theirs[:, i : i + 1] for i in range(3)]
        top = jnp.maximum(top1, top2)
        weight1 = jnp.exp2((top1 - top) * power)
        weight2 = jnp.exp2((top2 - top) * power)
        inverse = 1.0 / (total1 * weight1 + total2 * weight2)
        delta = (dot1 * weight1 + dot2 * weight2) * inverse
        return top, inverse, delta, weight1 * inverse, total2 * weight2 * inverse

    def first_pass(rs, qn, grad, keys, values):
        scores = [[dot_nt(a, key) for key in ks] for a, ks in zip(qn, keys)]
        top = [row_max(s) for s in scores]
        expo = [[jnp.exp2((x - t) * power) for x in s] for s, t in zip(scores, top)]
        total = [row_sum(e) for e in expo]
        summed = [weigh([x.astype(BF16) for x in e], val) for e, val in zip(expo, values)]
        for i, r in enumerate(rs):
            near_trip[r, :, 0:1] = top[i]
            near_trip[r, :, 1:2] = total[i]
            near_trip[r, :, 2:3] = row_sum([grad[i].astype(F32) * summed[i]])
        return summed, total

    def second_pass(qn, grad, keys, values, merge):
        scores = [[dot_nt(a, key) for key in ks] for a, ks in zip(qn, keys)]
        grad_probs = [[dot_nt(a, val) for val in vs] for a, vs in zip(grad, values)]
        probs = [[jnp.exp2((x - m[0]) * power) * m[1] for x in s] for s, m in zip(scores, merge)]
        grad_scores = [
            [(p * (d - m[2])).astype(BF16) for p, d in zip(ps, ds)] for ps, ds, m in zip(probs, grad_probs, merge)
        ]
        return probs, grad_scores, [weigh(s, key) * scaling for s, key in zip(grad_scores, keys)]

    def trade(p, target):
        lane = lax.broadcasted_iota(jnp.int32, (length, DH), 1)
        packed = jnp.zeros((length, DH), F32)
        for x, r in enumerate(batches[p]):
            for i in range(3):
                packed = jnp.where(lane == 4 * x + i, near_trip[r, :, i : i + 1], packed)
        rows = jnp.transpose(packed)
        for x, r in enumerate(batches[p]):
            trip_out[r] = rows[4 * x : 4 * x + 4]
        trip_copy(p, target).start()

    def traded(p, target):
        trip_copy(p, target).wait_recv()
        for r in batches[p]:
            far_trip[r, :, 0:4] = jnp.transpose(trip_in[r])

    def far_operands(r):
        cols = columns(kept + r)
        q_full = far[r, 0].astype(F32)
        rate, gain = far_wide[...], gq[:, cols]
        keys = [clean[j, 0, :, cols] for j in range(2)]
        values = [clean[j, 1, :, cols] for j in range(2)]
        return cols, q_full, rate, gain, (q_full * rate * gain).astype(BF16), far[r, 1], keys, values

    def near_operands(nb, r):
        cols = columns(kept + r)
        q_full = q[:, cols].astype(F32)
        k_full = k[:, cols].astype(F32)
        qn = (q_full * wide[0] * gq[:, cols]).astype(BF16)
        kn = (k_full * wide[1] * gk[:, cols]).astype(BF16)
        keys = [kn] + [clean[j, 0, :, cols] for j in range(2, nb)]
        values = [v[:, cols]] + [clean[j, 1, :, cols] for j in range(2, nb)]
        return cols, q_full, k_full, qn, g[:, cols], keys, values

    def help_first(nb, p):
        rs = batches[p]
        land = far.at[pl.ds(rs[0], len(rs))]
        frame_copy(land, land, far_send.at[0], far_recv.at[p], nb + 2).wait_recv()
        _, _, _, _, qn, grad, keys, values = zip(*[far_operands(r) for r in rs])
        summed, total = first_pass(rs, qn, grad, keys, values)
        for i, r in enumerate(rs):
            back_out[1, r] = (summed[i] / total[i]).astype(BF16)

    def help_second(rs):
        cols, q_full, rate, gain, qn, grad, keys, values = zip(*[far_operands(r) for r in rs])
        merge = [merged(near_trip[r], far_trip[r]) for r in rs]
        _, _, grad_qn = second_pass(qn, grad, keys, values, merge)
        for i, r in enumerate(rs):
            back_out[0, r] = grad_qn[i].astype(BF16)
            far_inner[...] += q_full[i] * (grad_qn[i] * gain[i])
            far_sums[r : r + 1, :] = jnp.sum(grad_qn[i] * q_full[i] * rate[i], axis=0, keepdims=True)

    def near_first(nb, rs):
        _, _, _, qn, grad, keys, values = zip(*[near_operands(nb, r) for r in rs])
        summed, _ = first_pass(rs, qn, grad, keys, values)
        for i, r in enumerate(rs):
            part[r] = summed[i]

    def near_second(nb, rs):
        cols, q_full, k_full, qn, grad, keys, values = zip(*[near_operands(nb, r) for r in rs])
        merge = [merged(near_trip[r], far_trip[r]) for r in rs]
        probs, grad_scores, grad_qn = second_pass(qn, grad, keys, values, merge)
        store_blocks(cols, q_full, k_full, qn, grad, grad_qn, grad_scores, probs)
        for m, r in zip(merge, rs):
            part[r] = part[r] * m[3]
            far_trip[r, :, 3:4] = m[4]

    def s1_copy(d, part):
        return pltpu.make_async_remote_copy(
            src_ref=part,
            dst_ref=part,
            send_sem=sum_send.at[0],
            recv_sem=sum_recv.at[0],
            device_id=peer1(d),
            device_id_type=MESH,
        )

    slots = 2 * videos if lent else n1
    high = me1 - n1 + slots

    def send_sums(addend):
        sums1[high] = sums[...] + addend
        repeat(1, n1, lambda d: s1_copy(d, sums1.at[high]).start())

    def end_copy(d, part):
        p = lax.rem((frame * fsdp + fs) * heads_axis + lax.axis_index("head") + d, devices)
        return pltpu.make_async_remote_copy(
            src_ref=part,
            dst_ref=part,
            send_sem=end_send.at[0],
            recv_sem=end_recv.at[0],
            device_id={
                "frame": p // (fsdp * heads_axis),
                "fsdp": lax.rem(p // heads_axis, fsdp),
                "head": lax.rem(p, heads_axis),
            },
            device_id_type=MESH,
        )

    last = pl.ds((kept - 1) * DH, 2 * DH)

    def own_range(nb, first, last):
        repeat(first // group, last // group, lambda i: own_heads(nb, [group * i + x for x in range(group)]))

    for nb in range(frames):

        @pl.when(frame == nb)
        def _():
            if nb % 2 == 1:
                partner_copy(nb - 1).wait_recv()
            if helps(nb):
                other = nb + 2
                own_range(nb, 0, head_count)
                if nb == 0:
                    partner_copy(1).wait_recv()
                row_copy(other).wait_recv()
                far_wide[...] = jnp.broadcast_to(jnp.transpose(row_in[...])[:, 0:1], (length, DH))
                far_inner[...] = jnp.zeros_like(far_inner)
                help_first(nb, 0)
                trade(0, other)
                send_own(nb, kept - 1, kept)
                traded(0, other)
                help_second(batches[0])
                back_copy(0, order[0], other).start()
                help_first(nb, 1)
                trade(1, other)
                traded(1, other)
                help_second(batches[1])
                for r in range(lent):
                    sums[0:1, columns(kept + r)] += far_sums[r : r + 1, :]
                sum_copy(other).start()
                row_out[...] = as_rows(far_inner[...], jnp.zeros_like(far_inner))[0:2]
                row_copy(other).start()
                for r in order[1:]:
                    back_copy(0, r, other).start()
                repeat(0, lent, lambda r: back_copy(1, r, other).start())
                stats_go(1, as_rows(inner_q[...], inner_k[...]))
            elif helped(nb):
                other = nb - 2
                for p in range(2):
                    near_first(nb, batches[p])
                    trade(p, other)

                sums[:, last] = jnp.zeros((2, 2 * DH), F32)

                def step(h):
                    pass_on(nb, h)

                    @pl.when(h == kept - 2)
                    def _():
                        traded(0, other)
                        near_second(nb, batches[0])

                    @pl.when(h == kept - 1)
                    def _():
                        sum_copy(other).wait_recv()
                        send_sums(far_sum[...])

                    own_heads(nb, [h])

                repeat(0, kept, step)
                traded(1, other)
                near_second(nb, batches[1])
                row_copy(other).wait_recv()
                rows = as_rows(inner_q[...], inner_k[...])
                stats_go(1, jnp.where(row == 0, rows + row_in[0:1], rows))
                end = me2 * slots + high
                ends[end] = sums[:, last]
                repeat(1, devices, lambda d: end_copy(d, ends.at[end]).start())
            else:

                def step(h):
                    pass_on(nb, h)
                    own_heads(nb, [h])

                repeat(0, head_count, step)
                send_sums(0.0)
                stats_go(1, as_rows(inner_q[...], inner_k[...]))

    def s2_copy(d, part):
        return pltpu.make_async_remote_copy(
            src_ref=part,
            dst_ref=part,
            send_sem=sum_send.at[1],
            recv_sem=sum_recv.at[1],
            device_id=peer2(d),
            device_id_type=MESH,
        )

    def only(which, action):
        for nb in range(frames):
            if which(nb):
                pl.when(frame == nb)(action)

    all_s2 = s2_copy(1, sums2.at[pl.ds(0, n2 - 1)])

    def finish_heads():
        inners = jnp.transpose(stats_total(1))
        for i, inner in enumerate((inner_q, inner_k)):
            full = jnp.broadcast_to(inners[:, i : i + 1], (length, DH))
            inner[...] = wide[i] * wide[i] * wide[i] * full / features

        def finish(h):
            cols = columns(h)
            dq_out[:, cols] = (wide[0] * flat_q[:, cols] - q[:, cols].astype(F32) * inner_q[...]).astype(BF16)
            dk_out[:, cols] = (wide[1] * flat_k[:, cols] - k[:, cols].astype(F32) * inner_k[...]).astype(BF16)

        repeat(0, head_count, finish)

    def gather_sums(count):
        s1_copy(1, sums1.at[pl.ds(0, count)]).wait_recv()
        sums2[me2] = jnp.sum(sums1[pl.ds(0, slots)], axis=0)
        for d in range(1, n2):
            s2_copy(d, sums2.at[me2]).start()

    if lent:

        @pl.when(frame < 2)
        def _():
            finish_heads()
            gather_sums(slots)

        @pl.when(frame >= 2)
        def _():
            gather_sums(slots - 1)
            grads = back_in.at[0]
            frame_copy(grads, grads, back_send.at[0], grad_recv.at[0], 0).wait_recv()

            def add(r):
                cols = columns(kept + r)
                flat_q[:, cols] += back_in[0, r].astype(F32) * gq[:, cols]

            repeat(0, lent, add)
            finish_heads()

    else:
        gather_sums(slots - 1)
        finish_heads()

    def only(which, action):
        for nb in range(frames):
            if which(nb):
                pl.when(frame == nb)(action)

    all_s2.wait_recv()
    for p in range(n2):
        gain_q_out[:, p * width : (p + 1) * width] = sums2[p, 0:1, :]
        gain_k_out[:, p * width : (p + 1) * width] = sums2[p, 1:2, :]
    if lent:
        only(helps, end_copy(1, ends.at[pl.ds(0, n2 * slots)]).wait_recv)
        only(helped, end_copy(1, ends.at[pl.ds(0, n2 * slots - 1)]).wait_recv)
        for p in range(n2):
            late = jnp.sum(ends[pl.ds(p * slots, slots)], axis=0)
            cols = pl.ds(p * width + (kept - 1) * DH, 2 * DH)
            gain_q_out[:, cols] += late[0:1]
            gain_k_out[:, cols] += late[1:2]

    for nb in range(frames):
        if helped(nb):

            @pl.when(frame == nb)
            def _():
                def join(r):
                    back_copy(1, r, nb - 2).wait_recv()
                    far = back_in[1, r].astype(F32) * far_trip[r, :, 3:4]
                    att_out[:, columns(kept + r)] = (part[r] + far).astype(BF16)

                repeat(0, lent, join)

    stats_copy(0, 1, stats.at[:, pl.ds(0, n2 - 1)]).wait_send()
    if lent:
        only(helped, s1_copy(1, sums1.at[pl.ds(0, n1 - 1)]).wait_send)
        only(helped, end_copy(1, ends.at[pl.ds(0, devices - 1)]).wait_send)
        only(helps, lambda: sum_copy(2).wait_send())
    else:
        s1_copy(1, sums1.at[pl.ds(0, n1 - 1)]).wait_send()
    all_s2.wait_send()
    for nb in range(frames):
        direct, _, _, further = plan(nb)

        @pl.when(frame == nb)
        def _():
            if further is not None:
                kept_heads(nb, own_send.at[0]).wait_send()
            if has_partner_copy(nb):
                partner_copy(nb).wait_send()
            for j in direct:
                for t in range(1 if further is None else 2):
                    kept_heads(j, relay_send.at[t, j // 2]).wait_send()
            if helps(nb) or helped(nb):
                other = nb + 2 if helps(nb) else nb - 2
                frame_copy(trip_out, trip_in, row_send.at[1], row_recv.at[1], other).wait_send()
                row_copy(other).wait_send()
            if helps(nb):
                frame_copy(back_out, back_in, back_send.at[0], grad_recv.at[0], nb + 2).wait_send()
            if helped(nb):
                frame_copy(far, far, far_send.at[0], far_recv.at[0], nb - 2).wait_send()


def write_out(*refs):
    sem = refs[12]
    copies = [pltpu.make_async_copy(refs[i], refs[6 + i], sem.at[i]) for i in range(6)]
    for copy in copies:
        copy.start()
    for copy in copies:
        copy.wait()


def on_device(queries, noisy_keys, noisy_values, clean_keys, clean_values, gain_query, gain_key, out_grad):
    length, width = queries.shape
    features = gain_query.shape[0]
    frames = lax.axis_size("frame")
    fsdp = lax.axis_size("fsdp")
    heads_axis = lax.axis_size("head")
    head_count = width // DH
    n1 = frames * (fsdp // 2)
    n2 = 2 * heads_axis
    block = pltpu.VMEM((length, width), BF16)
    gains = pltpu.VMEM((1, features), F32)
    anywhere = pl.BlockSpec(memory_space=pl.ANY)
    vmem = pl.BlockSpec(memory_space=pltpu.VMEM)
    dma = pltpu.SemaphoreType.DMA
    chips = max(frames // 2 - 1, 1)
    kept = 4 * 2 * length * width + 2 * 4 * features
    lent = head_count // 5 * 2 if frames == 4 and head_count >= 5 else 0
    held = max(lent, 1)
    kept_count = head_count - lent
    outs = pl.pallas_call(
        functools.partial(kernel, frames, fsdp, heads_axis, width, features, lent),
        out_shape=(block, block, block, block, gains, gains),
        in_specs=[anywhere] * 8,
        out_specs=[vmem] * 6,
        scratch_shapes=[
            pltpu.VMEM((4, length, width), BF16),
            pltpu.VMEM((2, 1, width), F32),
            pltpu.VMEM((frames, 2, length, width), BF16),
            pltpu.VMEM((length, width), F32),
            pltpu.VMEM((length, width), F32),
            pltpu.VMEM((length, DH), F32),
            pltpu.VMEM((length, DH), F32),
            pltpu.VMEM((2, length, DH), F32),
            pltpu.VMEM((2, n2, 8, length), F32),
            pltpu.VMEM((2, width), F32),
            pltpu.VMEM((n1, 2, width), F32),
            pltpu.VMEM((n2, 2, width), F32),
            pltpu.VMEM((frames * fsdp * heads_axis if lent else 1, 2, 2 * DH), F32),
            pltpu.VMEM((2, width), F32),
            pltpu.VMEM((held, 2, length, DH), BF16),
            pltpu.VMEM((length, DH), F32),
            pltpu.VMEM((length, DH), F32),
            pltpu.VMEM((-(-held // 8) * 8, DH), F32),
            pltpu.VMEM((held, length, DH), F32),
            pltpu.VMEM((2, held, length, DH), BF16),
            pltpu.VMEM((2, held, length, DH), BF16),
            pltpu.VMEM((held, length, 8), F32),
            pltpu.VMEM((held, length, 8), F32),
            pltpu.VMEM((held, 4, length), F32),
            pltpu.VMEM((held, 4, length), F32),
            pltpu.VMEM((2, length), F32),
            pltpu.VMEM((2, length), F32),
            dma((4,)),
            dma((2,)),
            dma((min(chips, 2), chips)),
            dma((chips, kept_count)),
            dma((chips, kept_count)),
            dma((1,)),
            dma((1,)),
            dma((2,)),
            dma((2,)),
            dma((2,)),
            dma((1,)),
            dma((2,)),
            dma((1,)),
            dma((1,)),
            dma((held,)),
            dma((3,)),
            dma((4,)),
            dma((1,)),
            dma((1,)),
            pltpu.SemaphoreType.REGULAR,
        ],
        compiler_params=pltpu.CompilerParams(
            collective_id=0, has_side_effects=True, vmem_limit_bytes=VMEM_BYTES - kept - 4096
        ),
        name="attention",
    )(
        queries, noisy_keys, noisy_values, clean_keys, clean_values,
        gain_query.reshape(1, features), gain_key.reshape(1, features), out_grad,
    )
    outs = pl.pallas_call(
        write_out,
        out_shape=tuple(jax.ShapeDtypeStruct(out.shape, out.dtype) for out in outs),
        in_specs=[anywhere] * 6,
        out_specs=[anywhere] * 6,
        scratch_shapes=[dma((6,))],
        compiler_params=pltpu.CompilerParams(vmem_limit_bytes=8 * 1024 * 1024),
        name="write_out",
    )(*outs)
    return (*outs[:4], outs[4].reshape(features), outs[5].reshape(features))


def solution(mesh):
    tokens = P("frame", ("fsdp", "head"))
    return jax.shard_map(
        on_device,
        mesh=mesh,
        in_specs=(tokens, tokens, tokens, tokens, tokens, P(), P(), tokens),
        out_specs=(tokens, tokens, tokens, tokens, P(), P()),
        check_vma=False,
    )
```

```python
import functools
import math

import jax
import jax.numpy as jnp
from jax import lax
from jax.experimental import pallas as pl
from jax.experimental.pallas import tpu as pltpu
from jax.sharding import PartitionSpec as P

DH = 128
EPSILON = 1e-06
MESH = pl.DeviceIdType.MESH
VMEM_BYTES = 67043328
F32 = jnp.float32
BF16 = jnp.bfloat16


def dot_nt(a, b):
    return lax.dot_general(a, b, (((1,), (1,)), ((), ())), preferred_element_type=F32)


def dot_nn(a, b):
    return lax.dot_general(a, b, (((1,), (0,)), ((), ())), preferred_element_type=F32)


def dot_tn(a, b):
    return lax.dot_general(a, b, (((0,), (0,)), ((), ())), preferred_element_type=F32)


def kernel(
    frames, fsdp, heads_axis, width, features, lent,
    q_hbm, k_hbm, v_hbm, ck_hbm, cv_hbm, gq_hbm, gk_hbm, g_hbm,
    att_out, dq_out, dk_out, dv_out, gain_q_out, gain_k_out,
    tokens, gains, clean, flat_q, flat_k, inner_q, inner_k, wide,
    stats, sums, sums1, sums2, ends, far_sum, far, far_wide, far_inner, far_sums, part, back_out, back_in,
    near_trip, far_trip, trip_out, trip_in, row_out, row_in,
    load_sem, own_send, relay_send, direct_recv, relay_recv, partner_recv, stats_send, stats_recv, sum_send, sum_recv,
    far_send, far_recv, back_send, grad_recv, att_recv, row_send, row_recv, end_send, end_recv, ready,
):
    q, k, v, g = [tokens.at[i] for i in range(4)]
    gq, gk = gains.at[0], gains.at[1]
    length = tokens.shape[1]
    head_count = width // DH
    devices = frames * fsdp * heads_axis
    kept = head_count - lent
    batches = [list(range(1, lent)), [0]]
    order = batches[0] + batches[1]
    group = 2 - head_count % 2
    videos = fsdp // 2
    scaling = 1.0 / math.sqrt(DH)
    power = scaling * math.log2(math.e)
    frame = lax.axis_index("frame")
    fs = lax.axis_index("fsdp")
    half = fs // videos
    video = lax.rem(fs, videos)
    me1 = frame * videos + video
    n1 = frames * videos
    me2 = half * heads_axis + lax.axis_index("head")
    n2 = 2 * heads_axis

    def peer1(distance):
        p = lax.rem(me1 + distance, n1)
        return {"frame": p // videos, "fsdp": half * videos + lax.rem(p, videos)}

    def peer2(distance):
        p = lax.rem(me2 + distance, n2)
        return {"fsdp": (p // heads_axis) * videos + video, "head": lax.rem(p, heads_axis)}

    def columns(h):
        return pl.ds(pl.multiple_of(h * DH, DH), DH)

    def repeat(first, last, step):
        def body(i, _):
            step(i)
            return 0

        lax.fori_loop(first, last, body, 0)

    def arrive(ref, sem):
        pltpu.make_async_copy(ref, ref, sem).wait()

    for nb in range(frames - 1):

        @pl.when(frame == nb)
        def _():
            for kv, src in enumerate((ck_hbm, cv_hbm)):
                pltpu.make_async_copy(src, clean.at[nb, kv], load_sem.at[3]).start()

    barrier = pltpu.get_barrier_semaphore()

    groups = videos - 1 + n2 - 1
    if lent:
        mates = [{"frame": jnp.int32(f)} for f in range(frames)]
        for f in range(frames):

            @pl.when(frame != f)
            def _():
                pl.semaphore_signal(barrier, inc=1, device_id=mates[f], device_id_type=MESH)

        for f in range(1, frames, 2):
            for d in range(1, videos):
                near = {"fsdp": half * videos + lax.rem(video + d, videos)}
                pl.semaphore_signal(barrier, inc=1, device_id={**near, **mates[f]}, device_id_type=MESH)
            for d in range(1, n2):
                pl.semaphore_signal(barrier, inc=1, device_id={**peer2(d), **mates[f]}, device_id_type=MESH)
    else:
        repeat(1, n1, lambda d: pl.semaphore_signal(barrier, inc=1, device_id=peer1(d), device_id_type=MESH))
        for d in range(1, n2):
            pl.semaphore_signal(barrier, inc=1, device_id=peer2(d), device_id_type=MESH)
    start = pl.multiple_of(me2 * width, DH)
    for src, dst, i in (
        (q_hbm, q, 0),
        (k_hbm, k, 0),
        (gq_hbm.at[:, pl.ds(start, width)], gq, 1),
        (gk_hbm.at[:, pl.ds(start, width)], gk, 1),
        (v_hbm, v, 2),
        (g_hbm, g, 2),
    ):
        pltpu.make_async_copy(src, dst, load_sem.at[i]).start()
    if lent:
        pl.semaphore_wait(barrier, frames - 1 + lax.rem(frame, 2) * (frames * groups))

        @pl.when(lax.rem(frame, 2) == 1)
        def _():
            pl.semaphore_signal(ready, inc=1, device_id={"frame": frame - 1}, device_id_type=MESH)

    else:
        pl.semaphore_wait(barrier, n1 - 1 + n2 - 1)

    def frame_copy(src, dst, send, recv, target):
        return pltpu.make_async_remote_copy(
            src_ref=src,
            dst_ref=dst,
            send_sem=send,
            recv_sem=recv,
            device_id={"frame": jnp.int32(target)},
            device_id_type=MESH,
        )

    def direct_copy(j, h, target, send):
        land = clean.at[j, :, :, columns(h)]
        return frame_copy(land, land, send, direct_recv.at[j // 2, h], target)

    def relay_copy(j, h, target, send):
        land = clean.at[j, :, :, columns(h)]
        return frame_copy(land, land, send, relay_recv.at[j // 2, h], target)

    def partner_copy(j):
        land = clean.at[j] if j % 2 == 0 else clean.at[j, :, :, pl.ds(kept * DH, lent * DH)]
        return frame_copy(land, land, own_send.at[1], partner_recv.at[0], 2 * (j // 2) + 1 - j % 2)

    def kept_heads(j, sem):
        land = clean.at[j, :, :, pl.ds(0, kept * DH)]
        return frame_copy(land, land, sem, partner_recv.at[0], (j + 1) % frames)

    def plan(nb):
        pair, side = nb // 2, nb % 2
        partner, further = 2 * pair + 1 - side, nb + 2
        direct = [2 * c + side for c in range(pair)]
        relayed = [2 * c + 1 - side for c in range(pair)]
        return direct, relayed, partner, further if further < frames else None

    def helps(nb):
        return lent > 0 and nb < 2

    def helped(nb):
        return lent > 0 and nb >= 2

    def has_partner_copy(nb):
        return nb % 2 == 0 or helps(nb)

    def send_own(nb, first, last):
        further = plan(nb)[3]
        repeat(first, last, lambda h: direct_copy(nb, h, further, own_send.at[0]).start())

    def far_copy(kind, r, target):
        src = (q_hbm, g_hbm)[kind].at[:, columns(kept + r)]
        return frame_copy(src, far.at[r, kind], far_send.at[0], far_recv.at[0 if r in batches[0] else 1], target)

    def back_copy(kind, r, target):
        recv = grad_recv.at[0] if kind == 0 else att_recv.at[r]
        return frame_copy(back_out.at[kind, r], back_in.at[kind, r], back_send.at[0], recv, target)

    def trip_copy(p, target):
        rs = pl.ds(batches[p][0], len(batches[p]))
        return frame_copy(trip_out.at[rs], trip_in.at[rs], row_send.at[1], row_recv.at[1 + p], target)

    def sum_copy(target):
        return frame_copy(sums, far_sum, row_send.at[2], row_recv.at[3], target)

    def row_copy(target):
        return frame_copy(row_out, row_in, row_send.at[0], row_recv.at[0], target)

    def lend(nb, first, last):
        for r in order[first:last]:
            for kind in range(2):
                far_copy(kind, r, nb - 2).start()

    for nb in range(frames):

        @pl.when(frame == nb)
        def _():
            if helped(nb):
                lend(nb, 0, lent // 2)
            if nb < frames - 1:
                arrive(clean.at[nb], load_sem.at[3])
            if plan(nb)[3] is not None:
                send_own(nb, 0, kept - 1 if helps(nb) else kept)
            if has_partner_copy(nb):
                partner_copy(nb).start()

    row = lax.broadcasted_iota(jnp.int32, (8, length), 0)

    def as_rows(a, b):
        a = jnp.sum(jnp.transpose(a), axis=0, keepdims=True)
        b = jnp.sum(jnp.transpose(b), axis=0, keepdims=True)
        return jnp.where(row == 0, a, jnp.where(row == 1, b, 0.0))

    def stats_copy(phase, d, part):
        return pltpu.make_async_remote_copy(
            src_ref=part,
            dst_ref=part,
            send_sem=stats_send.at[0],
            recv_sem=stats_recv.at[phase],
            device_id=peer2(d),
            device_id_type=MESH,
        )

    def all_stats(phase):
        return stats_copy(phase, 1, stats.at[phase, pl.ds(0, n2 - 1)])

    def stats_go(phase, value):
        stats[phase, me2] = value
        for d in range(1, n2):
            stats_copy(phase, d, stats.at[phase, me2]).start()

    def stats_total(phase):
        all_stats(phase).wait_recv()
        return jnp.sum(stats[phase], axis=0)

    arrive(tokens.at[pl.ds(0, 2)], load_sem.at[0])

    def square(ref):
        total = jnp.zeros((length, DH), F32)
        for h in range(head_count):
            x = ref[:, h * DH : (h + 1) * DH].astype(F32)
            total = total + x * x
        return total

    if lent:

        @pl.when(lax.rem(frame, 2) == 0)
        def _():
            pl.semaphore_wait(ready, 1)

    stats_go(0, as_rows(square(q), square(k)))
    inner_q[...] = jnp.zeros_like(inner_q)
    inner_k[...] = jnp.zeros_like(inner_k)
    arrive(gains, load_sem.at[1])
    arrive(tokens.at[pl.ds(2, 2)], load_sem.at[2])
    rate_rows = lax.rsqrt(stats_total(0) / features + EPSILON)
    rate_columns = jnp.transpose(rate_rows)
    for i in range(2):
        wide[i] = jnp.broadcast_to(rate_columns[:, i : i + 1], (length, DH))
    for nb in range(frames):
        if helped(nb):

            @pl.when(frame == nb)
            def _():
                row_out[...] = rate_rows[0:2]
                row_copy(nb - 2).start()
                lend(nb, lent // 2, lent)

    def store_grads(cols, q_full, k_full, grad_qn, grad_kn):
        fq = grad_qn * gq[:, cols]
        fk = grad_kn * gk[:, cols]
        flat_q[:, cols] = fq
        flat_k[:, cols] = fk
        inner_q[...] += q_full * fq
        inner_k[...] += k_full * fk
        sums[0:1, cols] = jnp.sum(grad_qn * q_full * wide[0], axis=0, keepdims=True)
        sums[1:2, cols] = jnp.sum(grad_kn * k_full * wide[1], axis=0, keepdims=True)

    def pass_on(nb, h):
        direct, _, partner, further = plan(nb)
        for j in direct:
            direct_copy(j, h, partner, relay_send.at[0, j // 2]).wait_recv()
            relay_copy(j, h, partner, relay_send.at[0, j // 2]).start()
            if further is not None:
                direct_copy(j, h, further, relay_send.at[1, j // 2]).start()

    def row_sum(terms):
        return functools.reduce(jnp.add, [jnp.sum(t, axis=1, keepdims=True) for t in terms])

    def row_max(terms):
        return functools.reduce(jnp.maximum, [jnp.max(t, axis=1, keepdims=True) for t in terms])

    def weigh(blocks, operands):
        return functools.reduce(jnp.add, [dot_nn(b, o) for b, o in zip(blocks, operands)])

    def own_heads(nb, hs):
        _, relayed, partner, _ = plan(nb)
        cols = [columns(h) for h in hs]
        q_full = [q[:, c].astype(F32) for c in cols]
        k_full = [k[:, c].astype(F32) for c in cols]
        qn = [(x * wide[0] * gq[:, c]).astype(BF16) for x, c in zip(q_full, cols)]
        kn = [(x * wide[1] * gk[:, c]).astype(BF16) for x, c in zip(k_full, cols)]
        grad = [g[:, c] for c in cols]
        scores = [[dot_nt(a, b)] for a, b in zip(qn, kn)]
        grad_probs = [[dot_nt(a, v[:, c])] for a, c in zip(grad, cols)]
        for h in hs:
            for j in relayed:
                relay_copy(j, h, partner, relay_send.at[0, j // 2]).wait_recv()
        keys = [[b] + [clean[j, 0, :, c] for j in range(nb)] for b, c in zip(kn, cols)]
        values = [[v[:, c]] + [clean[j, 1, :, c] for j in range(nb)] for c in cols]
        for i in range(len(hs)):
            scores[i] += [dot_nt(qn[i], key) for key in keys[i][1:]]
            grad_probs[i] += [dot_nt(grad[i], val) for val in values[i][1:]]
        top = [row_max(s) for s in scores]
        expo = [[jnp.exp2((x - t) * power) for x in s] for s, t in zip(scores, top)]
        inverse = [1.0 / row_sum(e) for e in expo]
        summed = [weigh([x.astype(BF16) for x in e], val) for e, val in zip(expo, values)]
        attention = [s * i for s, i in zip(summed, inverse)]
        for c, a in zip(cols, attention):
            att_out[:, c] = a.astype(BF16)
        delta = [row_sum([x.astype(F32) * a]) for x, a in zip(grad, attention)]
        probs = [[x * i for x in e] for e, i in zip(expo, inverse)]
        grad_scores = [
            [(p * (d - x)).astype(BF16) for p, d in zip(ps, ds)] for ps, ds, x in zip(probs, grad_probs, delta)
        ]
        grad_qn = [weigh(s, key) * scaling for s, key in zip(grad_scores, keys)]
        store_blocks(cols, q_full, k_full, qn, grad, grad_qn, grad_scores, probs)

    def store_blocks(cols, q_full, k_full, qn, grad, grad_qn, grad_scores, probs):
        grad_kn = [dot_tn(s[0], a) * scaling for s, a in zip(grad_scores, qn)]
        grad_v = [dot_tn(p[0].astype(BF16), x) for p, x in zip(probs, grad)]
        for c, x in zip(cols, grad_v):
            dv_out[:, c] = x.astype(BF16)
        for args in zip(cols, q_full, k_full, grad_qn, grad_kn):
            store_grads(*args)

    def merged(mine, theirs):
        top1, total1, dot1 = [mine[:, i : i + 1] for i in range(3)]
        top2, total2, dot2 = [theirs[:, i : i + 1] for i in range(3)]
        top = jnp.maximum(top1, top2)
        weight1 = jnp.exp2((top1 - top) * power)
        weight2 = jnp.exp2((top2 - top) * power)
        inverse = 1.0 / (total1 * weight1 + total2 * weight2)
        delta = (dot1 * weight1 + dot2 * weight2) * inverse
        return top, inverse, delta, weight1 * inverse, total2 * weight2 * inverse

    def first_pass(rs, qn, grad, keys, values):
        scores = [[dot_nt(a, key) for key in ks] for a, ks in zip(qn, keys)]
        top = [row_max(s) for s in scores]
        expo = [[jnp.exp2((x - t) * power) for x in s] for s, t in zip(scores, top)]
        total = [row_sum(e) for e in expo]
        summed = [weigh([x.astype(BF16) for x in e], val) for e, val in zip(expo, values)]
        for i, r in enumerate(rs):
            near_trip[r, :, 0:1] = top[i]
            near_trip[r, :, 1:2] = total[i]
            near_trip[r, :, 2:3] = row_sum([grad[i].astype(F32) * summed[i]])
        return summed, total

    def second_pass(qn, grad, keys, values, merge):
        scores = [[dot_nt(a, key) for key in ks] for a, ks in zip(qn, keys)]
        grad_probs = [[dot_nt(a, val) for val in vs] for a, vs in zip(grad, values)]
        probs = [[jnp.exp2((x - m[0]) * power) * m[1] for x in s] for s, m in zip(scores, merge)]
        grad_scores = [
            [(p * (d - m[2])).astype(BF16) for p, d in zip(ps, ds)] for ps, ds, m in zip(probs, grad_probs, merge)
        ]
        return probs, grad_scores, [weigh(s, key) * scaling for s, key in zip(grad_scores, keys)]

    def trade(p, target):
        lane = lax.broadcasted_iota(jnp.int32, (length, DH), 1)
        packed = jnp.zeros((length, DH), F32)
        for x, r in enumerate(batches[p]):
            for i in range(3):
                packed = jnp.where(lane == 4 * x + i, near_trip[r, :, i : i + 1], packed)
        rows = jnp.transpose(packed)
        for x, r in enumerate(batches[p]):
            trip_out[r] = rows[4 * x : 4 * x + 4]
        trip_copy(p, target).start()

    def traded(p, target):
        trip_copy(p, target).wait_recv()
        for r in batches[p]:
            far_trip[r, :, 0:4] = jnp.transpose(trip_in[r])

    def far_operands(r):
        cols = columns(kept + r)
        q_full = far[r, 0].astype(F32)
        rate, gain = far_wide[...], gq[:, cols]
        keys = [clean[j, 0, :, cols] for j in range(2)]
        values = [clean[j, 1, :, cols] for j in range(2)]
        return cols, q_full, rate, gain, (q_full * rate * gain).astype(BF16), far[r, 1], keys, values

    def near_operands(nb, r):
        cols = columns(kept + r)
        q_full = q[:, cols].astype(F32)
        k_full = k[:, cols].astype(F32)
        qn = (q_full * wide[0] * gq[:, cols]).astype(BF16)
        kn = (k_full * wide[1] * gk[:, cols]).astype(BF16)
        keys = [kn] + [clean[j, 0, :, cols] for j in range(2, nb)]
        values = [v[:, cols]] + [clean[j, 1, :, cols] for j in range(2, nb)]
        return cols, q_full, k_full, qn, g[:, cols], keys, values

    def help_first(nb, p):
        rs = batches[p]
        land = far.at[pl.ds(rs[0], len(rs))]
        frame_copy(land, land, far_send.at[0], far_recv.at[p], nb + 2).wait_recv()
        _, _, _, _, qn, grad, keys, values = zip(*[far_operands(r) for r in rs])
        summed, total = first_pass(rs, qn, grad, keys, values)
        for i, r in enumerate(rs):
            back_out[1, r] = (summed[i] / total[i]).astype(BF16)

    def help_second(rs):
        cols, q_full, rate, gain, qn, grad, keys, values = zip(*[far_operands(r) for r in rs])
        merge = [merged(near_trip[r], far_trip[r]) for r in rs]
        _, _, grad_qn = second_pass(qn, grad, keys, values, merge)
        for i, r in enumerate(rs):
            back_out[0, r] = grad_qn[i].astype(BF16)
            far_inner[...] += q_full[i] * (grad_qn[i] * gain[i])
            far_sums[r : r + 1, :] = jnp.sum(grad_qn[i] * q_full[i] * rate[i], axis=0, keepdims=True)

    def near_first(nb, rs):
        _, _, _, qn, grad, keys, values = zip(*[near_operands(nb, r) for r in rs])
        summed, _ = first_pass(rs, qn, grad, keys, values)
        for i, r in enumerate(rs):
            part[r] = summed[i]

    def near_second(nb, rs):
        cols, q_full, k_full, qn, grad, keys, values = zip(*[near_operands(nb, r) for r in rs])
        merge = [merged(near_trip[r], far_trip[r]) for r in rs]
        probs, grad_scores, grad_qn = second_pass(qn, grad, keys, values, merge)
        store_blocks(cols, q_full, k_full, qn, grad, grad_qn, grad_scores, probs)
        for m, r in zip(merge, rs):
            part[r] = part[r] * m[3]
            far_trip[r, :, 3:4] = m[4]

    def s1_copy(d, part):
        return pltpu.make_async_remote_copy(
            src_ref=part,
            dst_ref=part,
            send_sem=sum_send.at[0],
            recv_sem=sum_recv.at[0],
            device_id=peer1(d),
            device_id_type=MESH,
        )

    slots = 2 * videos if lent else n1
    high = me1 - n1 + slots

    def send_sums(addend):
        sums1[high] = sums[...] + addend
        repeat(1, n1, lambda d: s1_copy(d, sums1.at[high]).start())

    def end_copy(target, part):
        return pltpu.make_async_remote_copy(
            src_ref=part,
            dst_ref=part,
            send_sem=end_send.at[0],
            recv_sem=end_recv.at[0],
            device_id=target,
            device_id_type=MESH,
        )

    def send_ends(part):
        rows = [lax.rem(frame + a, frames) for a in range(frames)]
        heads = [lax.rem(lax.axis_index("head") + c, heads_axis) for c in range(heads_axis)]

        def column(b, skip):
            at = lax.rem(fs + b, fsdp)
            for a, c in [(a, c) for a in range(frames) for c in range(heads_axis)][skip:]:
                end_copy({"frame": rows[a], "fsdp": at, "head": heads[c]}, part).start()

        repeat(1, fsdp, lambda b: column(b, 0))
        column(0, 1)

    last = pl.ds((kept - 1) * DH, 2 * DH)

    def own_range(nb, first, last):
        repeat(first // group, last // group, lambda i: own_heads(nb, [group * i + x for x in range(group)]))

    for nb in range(frames):

        @pl.when(frame == nb)
        def _():
            if nb % 2 == 1:
                partner_copy(nb - 1).wait_recv()
            if helps(nb):
                other = nb + 2
                own_range(nb, 0, head_count)
                if nb == 0:
                    partner_copy(1).wait_recv()
                row_copy(other).wait_recv()
                far_wide[...] = jnp.broadcast_to(jnp.transpose(row_in[...])[:, 0:1], (length, DH))
                far_inner[...] = jnp.zeros_like(far_inner)
                help_first(nb, 0)
                trade(0, other)
                send_own(nb, kept - 1, kept)
                traded(0, other)
                help_second(batches[0])
                back_copy(0, order[0], other).start()
                help_first(nb, 1)
                trade(1, other)
                traded(1, other)
                help_second(batches[1])
                for r in range(lent):
                    sums[0:1, columns(kept + r)] += far_sums[r : r + 1, :]
                sum_copy(other).start()
                row_out[...] = as_rows(far_inner[...], jnp.zeros_like(far_inner))[0:2]
                row_copy(other).start()
                for r in order[1:]:
                    back_copy(0, r, other).start()
                repeat(0, lent, lambda r: back_copy(1, r, other).start())
                stats_go(1, as_rows(inner_q[...], inner_k[...]))
            elif helped(nb):
                other = nb - 2
                for p in range(2):
                    near_first(nb, batches[p])
                    trade(p, other)

                sums[:, last] = jnp.zeros((2, 2 * DH), F32)

                def step(h):
                    pass_on(nb, h)

                    @pl.when(h == kept - 2)
                    def _():
                        traded(0, other)
                        near_second(nb, batches[0])

                    @pl.when(h == kept - 1)
                    def _():
                        sum_copy(other).wait_recv()
                        send_sums(far_sum[...])

                    own_heads(nb, [h])

                repeat(0, kept, step)
                traded(1, other)
                near_second(nb, batches[1])
                end = me2 * slots + high
                ends[end] = sums[:, last]
                send_ends(ends.at[end])
                row_copy(other).wait_recv()
                rows = as_rows(inner_q[...], inner_k[...])
                stats_go(1, jnp.where(row == 0, rows + row_in[0:1], rows))
            else:

                def step(h):
                    pass_on(nb, h)
                    own_heads(nb, [h])

                repeat(0, head_count, step)
                send_sums(0.0)
                stats_go(1, as_rows(inner_q[...], inner_k[...]))

    def s2_copy(d, part):
        return pltpu.make_async_remote_copy(
            src_ref=part,
            dst_ref=part,
            send_sem=sum_send.at[1],
            recv_sem=sum_recv.at[1],
            device_id=peer2(d),
            device_id_type=MESH,
        )

    def only(which, action):
        for nb in range(frames):
            if which(nb):
                pl.when(frame == nb)(action)

    all_s2 = s2_copy(1, sums2.at[pl.ds(0, n2 - 1)])

    def finish_heads():
        inners = jnp.transpose(stats_total(1))
        for i, inner in enumerate((inner_q, inner_k)):
            full = jnp.broadcast_to(inners[:, i : i + 1], (length, DH))
            inner[...] = wide[i] * wide[i] * wide[i] * full / features

        def finish(h):
            cols = columns(h)
            dq_out[:, cols] = (wide[0] * flat_q[:, cols] - q[:, cols].astype(F32) * inner_q[...]).astype(BF16)
            dk_out[:, cols] = (wide[1] * flat_k[:, cols] - k[:, cols].astype(F32) * inner_k[...]).astype(BF16)

        repeat(0, head_count, finish)

    def gather_sums(count):
        s1_copy(1, sums1.at[pl.ds(0, count)]).wait_recv()
        sums2[me2] = jnp.sum(sums1[pl.ds(0, slots)], axis=0)
        for d in range(1, n2):
            s2_copy(d, sums2.at[me2]).start()

    if lent:

        @pl.when(frame < 2)
        def _():
            finish_heads()
            gather_sums(slots)

        @pl.when(frame >= 2)
        def _():
            gather_sums(slots - 1)
            grads = back_in.at[0]
            frame_copy(grads, grads, back_send.at[0], grad_recv.at[0], 0).wait_recv()

            def add(r):
                cols = columns(kept + r)
                flat_q[:, cols] += back_in[0, r].astype(F32) * gq[:, cols]

            repeat(0, lent, add)
            finish_heads()

    else:
        gather_sums(slots - 1)
        finish_heads()

    def only(which, action):
        for nb in range(frames):
            if which(nb):
                pl.when(frame == nb)(action)

    all_s2.wait_recv()
    for p in range(n2):
        gain_q_out[:, p * width : (p + 1) * width] = sums2[p, 0:1, :]
        gain_k_out[:, p * width : (p + 1) * width] = sums2[p, 1:2, :]
    if lent:
        only(helps, end_copy(peer2(1), ends.at[pl.ds(0, n2 * slots)]).wait_recv)
        only(helped, end_copy(peer2(1), ends.at[pl.ds(0, n2 * slots - 1)]).wait_recv)
        for p in range(n2):
            late = jnp.sum(ends[pl.ds(p * slots, slots)], axis=0)
            cols = pl.ds(p * width + (kept - 1) * DH, 2 * DH)
            gain_q_out[:, cols] += late[0:1]
            gain_k_out[:, cols] += late[1:2]

    for nb in range(frames):
        if helped(nb):

            @pl.when(frame == nb)
            def _():
                def join(r):
                    back_copy(1, r, nb - 2).wait_recv()
                    far = back_in[1, r].astype(F32) * far_trip[r, :, 3:4]
                    att_out[:, columns(kept + r)] = (part[r] + far).astype(BF16)

                repeat(0, lent, join)

    stats_copy(0, 1, stats.at[:, pl.ds(0, n2 - 1)]).wait_send()
    if lent:
        only(helped, s1_copy(1, sums1.at[pl.ds(0, n1 - 1)]).wait_send)
        only(helped, end_copy(peer2(1), ends.at[pl.ds(0, devices - 1)]).wait_send)
        only(helps, lambda: sum_copy(2).wait_send())
    else:
        s1_copy(1, sums1.at[pl.ds(0, n1 - 1)]).wait_send()
    all_s2.wait_send()
    for nb in range(frames):
        direct, _, _, further = plan(nb)

        @pl.when(frame == nb)
        def _():
            if further is not None:
                kept_heads(nb, own_send.at[0]).wait_send()
            if has_partner_copy(nb):
                partner_copy(nb).wait_send()
            for j in direct:
                for t in range(1 if further is None else 2):
                    kept_heads(j, relay_send.at[t, j // 2]).wait_send()
            if helps(nb) or helped(nb):
                other = nb + 2 if helps(nb) else nb - 2
                frame_copy(trip_out, trip_in, row_send.at[1], row_recv.at[1], other).wait_send()
                row_copy(other).wait_send()
            if helps(nb):
                frame_copy(back_out, back_in, back_send.at[0], grad_recv.at[0], nb + 2).wait_send()
            if helped(nb):
                frame_copy(far, far, far_send.at[0], far_recv.at[0], nb - 2).wait_send()


def write_out(*refs):
    sem = refs[12]
    copies = [pltpu.make_async_copy(refs[i], refs[6 + i], sem.at[i]) for i in range(6)]
    for copy in copies:
        copy.start()
    for copy in copies:
        copy.wait()


def on_device(queries, noisy_keys, noisy_values, clean_keys, clean_values, gain_query, gain_key, out_grad):
    length, width = queries.shape
    features = gain_query.shape[0]
    frames = lax.axis_size("frame")
    fsdp = lax.axis_size("fsdp")
    heads_axis = lax.axis_size("head")
    head_count = width // DH
    n1 = frames * (fsdp // 2)
    n2 = 2 * heads_axis
    block = pltpu.VMEM((length, width), BF16)
    gains = pltpu.VMEM((1, features), F32)
    anywhere = pl.BlockSpec(memory_space=pl.ANY)
    vmem = pl.BlockSpec(memory_space=pltpu.VMEM)
    dma = pltpu.SemaphoreType.DMA
    chips = max(frames // 2 - 1, 1)
    kept = 4 * 2 * length * width + 2 * 4 * features
    lent = head_count // 5 * 2 if frames == 4 and head_count >= 5 else 0
    held = max(lent, 1)
    kept_count = head_count - lent
    outs = pl.pallas_call(
        functools.partial(kernel, frames, fsdp, heads_axis, width, features, lent),
        out_shape=(block, block, block, block, gains, gains),
        in_specs=[anywhere] * 8,
        out_specs=[vmem] * 6,
        scratch_shapes=[
            pltpu.VMEM((4, length, width), BF16),
            pltpu.VMEM((2, 1, width), F32),
            pltpu.VMEM((frames, 2, length, width), BF16),
            pltpu.VMEM((length, width), F32),
            pltpu.VMEM((length, width), F32),
            pltpu.VMEM((length, DH), F32),
            pltpu.VMEM((length, DH), F32),
            pltpu.VMEM((2, length, DH), F32),
            pltpu.VMEM((2, n2, 8, length), F32),
            pltpu.VMEM((2, width), F32),
            pltpu.VMEM((n1, 2, width), F32),
            pltpu.VMEM((n2, 2, width), F32),
            pltpu.VMEM((frames * fsdp * heads_axis if lent else 1, 2, 2 * DH), F32),
            pltpu.VMEM((2, width), F32),
            pltpu.VMEM((held, 2, length, DH), BF16),
            pltpu.VMEM((length, DH), F32),
            pltpu.VMEM((length, DH), F32),
            pltpu.VMEM((-(-held // 8) * 8, DH), F32),
            pltpu.VMEM((held, length, DH), F32),
            pltpu.VMEM((2, held, length, DH), BF16),
            pltpu.VMEM((2, held, length, DH), BF16),
            pltpu.VMEM((held, length, 8), F32),
            pltpu.VMEM((held, length, 8), F32),
            pltpu.VMEM((held, 4, length), F32),
            pltpu.VMEM((held, 4, length), F32),
            pltpu.VMEM((2, length), F32),
            pltpu.VMEM((2, length), F32),
            dma((4,)),
            dma((2,)),
            dma((min(chips, 2), chips)),
            dma((chips, kept_count)),
            dma((chips, kept_count)),
            dma((1,)),
            dma((1,)),
            dma((2,)),
            dma((2,)),
            dma((2,)),
            dma((1,)),
            dma((2,)),
            dma((1,)),
            dma((1,)),
            dma((held,)),
            dma((3,)),
            dma((4,)),
            dma((1,)),
            dma((1,)),
            pltpu.SemaphoreType.REGULAR,
        ],
        compiler_params=pltpu.CompilerParams(
            collective_id=0, has_side_effects=True, vmem_limit_bytes=VMEM_BYTES - kept - 4096
        ),
        name="attention",
    )(
        queries, noisy_keys, noisy_values, clean_keys, clean_values,
        gain_query.reshape(1, features), gain_key.reshape(1, features), out_grad,
    )
    outs = pl.pallas_call(
        write_out,
        out_shape=tuple(jax.ShapeDtypeStruct(out.shape, out.dtype) for out in outs),
        in_specs=[anywhere] * 6,
        out_specs=[anywhere] * 6,
        scratch_shapes=[dma((6,))],
        compiler_params=pltpu.CompilerParams(vmem_limit_bytes=8 * 1024 * 1024),
        name="write_out",
    )(*outs)
    return (*outs[:4], outs[4].reshape(features), outs[5].reshape(features))


def solution(mesh):
    tokens = P("frame", ("fsdp", "head"))
    return jax.shard_map(
        on_device,
        mesh=mesh,
        in_specs=(tokens, tokens, tokens, tokens, tokens, P(), P(), tokens),
        out_specs=(tokens, tokens, tokens, tokens, P(), P()),
        check_vma=False,
    )
```
